128 devices in a mesh: aa: 8 (over z, core), ba: 4 (over y), col: 4 (over x).
Axes of the slice: x: 4, y: 4, z: 4, core: 2. Of those that a mesh axis runs over, the one named last changes fastest.
Arguments:
- tokens: bfloat16 [4096, 7168], P(('aa', 'col'), 'ba'), may hold values from -6 to 6
- routing: int32 [4096, 8], P(('aa', 'col')), may hold values from 0 to 31, all different within a row; in each aligned block of 128 rows (0 to 127, 128 to 255, ...) at most 40 rows name the same one
- gate_codes: int32 [4096, 8], P(('aa', 'col')), may hold values from 1 to 65535
- w_gate: bfloat16 [32, 7168, 2048], P(('aa', 'col'), None, 'ba'), may hold values from -0.0625 to 0.0625
- w_up: bfloat16 [32, 7168, 2048], P(('aa', 'col'), None, 'ba'), may hold values from -0.0625 to 0.0625
- w_down: bfloat16 [32, 2048, 7168], P(('aa', 'col'), 'ba'), may hold values from -0.125 to 0.125
Outputs:
- mixed: bfloat16 [4096, 7168], P(('aa', 'col'), 'ba')
The draws below stay inside these ranges and needn't reach their ends.
Inputs may be any that keep to these rules, and one draw needn't show every extreme that they name: `routing`: within each token group of 128 rows (aligned blocks of the rows), no expert is named more than 40 times, a bound that some block reaches. A token names 8 different experts.
All inputs are finite; a program needn't handle non-finite values.
Results may differ from the reference program's by a relative error of at most 0.014.
Values may be sent and summed in bfloat16 or wider, within the bound.
A program may use at most 192 MiB of HBM per device.

```python
import math
import jax
import jax.numpy as jnp
import numpy as np
from jax import lax

D = 7168
FF = 2048
TOP = 8
TOK_DEV = 128
EXPERTS = 32
TOKENS = 4096
CAP = 40
N_AA = 8
N_BA = 4
N_COL = 4


def touch_ends(entries, stream_key, low, top_value):
    extent = entries.shape
    place = [jax.random.randint(jax.random.fold_in(stream_key, axis), (), 0, extent[axis]) for axis in range(len(extent))]
    entries = entries.at[tuple(place)].set(low)
    longest = extent.index(max(extent))
    place[longest] = (place[longest] + 1) % extent[longest]
    return entries.at[tuple(place)].set(top_value)


def shard_levels(own_key, extent, pieces, least, high):
    loudness = 1.0
    for position, shards_of in pieces:
        heights = jax.random.uniform(jax.random.fold_in(jax.random.fold_in(own_key, 6), position), (shards_of,), jnp.float32, least / len(pieces), high / len(pieces))
        loudness = loudness * jnp.repeat(jnp.exp(heights), extent[position] // shards_of).reshape((-1,) + (1,) * (len(extent) - 1 - position))
    return loudness


def shared_out(own_key, own, number, rows, amount, top, bound, lean):
    order = jax.random.permutation(own_key, amount)
    crowded, usual = shares(amount, rows * top, bound, lean, True), shares(amount, rows * top, bound, lean, False)
    places = jnp.arange(amount)

    def named(sizes, turn):
        used = int((sizes > 0).sum())
        fixed = max(1, used // 4)
        shifted = fixed + (places - fixed + turn * (used - fixed)) % max(1, amount - fixed)
        return jnp.zeros((amount,), jnp.int32).at[order[jnp.where(places < fixed, places, shifted)]].set(jnp.asarray(sizes, jnp.int32))

    sizes = jnp.where(number % 4 == 0, named(crowded, number // 4), named(usual, number - number // 4 - 1))
    mixed = jax.random.permutation(jax.random.fold_in(own, 3), amount)
    giver, taker = mixed[0:amount // 2 * 2:2], mixed[1:amount // 2 * 2:2]
    margin = jnp.minimum(sizes[giver] - 1, bound - sizes[taker]) // 2
    margin = jnp.where((giver == order[0]) | (taker == order[0]) | (sizes[taker] == 0), 0, jnp.maximum(margin, 0))
    shifted = jax.random.randint(jax.random.fold_in(own, 4), (amount // 2,), 0, 1 << 20) % (margin + 1)
    sizes = sizes.at[giver].add(-shifted).at[taker].add(shifted)
    items = jnp.searchsorted(jnp.cumsum(sizes), jnp.arange(rows * top), side="right").astype(jnp.int32)
    listing = items.reshape(top, rows).T
    listing = listing[jax.random.permutation(jax.random.fold_in(own, 1), rows)]
    turn = jax.random.randint(jax.random.fold_in(own, 2), (rows, 1), 0, top)
    return jnp.take_along_axis(listing, (jnp.arange(top)[None, :] + turn) % top, axis=1)


def shares(amount, total, reach, skew, full):
    loads = [(1 << 20) // math.isqrt(grade ** skew) + 1 for grade in range(1, amount + 1)]
    largest = reach if full else min(reach, max(-(-total // amount), total * loads[0] // sum(loads)))
    least = 1 if total - largest >= amount - 1 else 0
    holding, spare = [largest] + [least] * (amount - 1), total - largest - least * (amount - 1)
    while spare > 0:
        free = [i for i in range(1, amount) if holding[i] < largest] or [i for i in range(1, amount) if holding[i] < reach]
        mass, budget = sum([loads[i] for i in free]), spare
        for i in free:
            more = min(reach - holding[i], max(1, budget * loads[i] // mass), spare)
            holding[i] = holding[i] + more
            spare = spare - more
    return np.array(holding)


def noise(stream_key, dims, spread, bound, shards=(), held_as=jnp.bfloat16):
    array = jax.random.normal(stream_key, dims, jnp.float32) * spread
    if len(shards) > 0:
        array = shard_levels(stream_key, dims, shards, -0.22, 0.18) * array
    return jnp.clip(array, min=-bound, max=bound).astype(held_as)


def setup_inputs(seed: int = 0) -> dict:
    key_of = jax.random.split(jax.random.key(seed), 7)
    tokens = noise(key_of[0], (TOKENS, D), 1.0, 6.0, ((0, 32), (1, 4)))
    routing_keys = jax.random.split(jax.random.fold_in(key_of[1], 1), TOKENS // TOK_DEV)
    routing_turns = jax.random.permutation(jax.random.fold_in(key_of[1], 3), TOKENS // TOK_DEV)
    routing = jax.vmap(lambda own, number: shared_out(jax.random.fold_in(key_of[1], 2), own, number, TOK_DEV, EXPERTS, TOP, CAP, 2))(routing_keys, routing_turns).reshape((TOKENS, TOP))
    gate_codes = touch_ends(jax.random.randint(key_of[2], (TOKENS, TOP), 1, 65536), jax.random.fold_in(key_of[2], 1), 1, 65535).astype(jnp.int32)
    w_gate = noise(key_of[3], (EXPERTS, D, FF), D ** -0.5, 0.0625, ((0, 32), (2, 4)))
    w_up = noise(key_of[4], (EXPERTS, D, FF), D ** -0.5, 0.0625, ((0, 32), (2, 4)))
    w_down = noise(key_of[5], (EXPERTS, FF, D), FF ** -0.5, 0.125, ((0, 32), (1, 4)))
    return {"tokens": tokens, "routing": routing, "gate_codes": gate_codes, "w_gate": w_gate, "w_up": w_up, "w_down": w_down}


route_scale = 2.827


def slot_tables(group_routes):
    flat = group_routes.reshape(-1)
    onehot = (flat[:, None] == jnp.arange(EXPERTS, dtype=jnp.int32)[None, :]).astype(jnp.int32)
    before = jnp.cumsum(onehot, axis=0) - onehot
    pos = jnp.sum(before * onehot, axis=1).astype(jnp.int32)
    slot = (flat * CAP + pos).astype(jnp.int32)
    matched = slot[:, None] == jnp.arange(EXPERTS * CAP, dtype=jnp.int32)[None, :]
    owner = (jnp.arange(flat.shape[0], dtype=jnp.int32) // TOP).astype(jnp.int32)
    slot_token = jnp.sum(jnp.where(matched, owner[:, None], 0), axis=0).astype(jnp.int32)
    live = jnp.any(matched, axis=0)
    return slot, slot_token.reshape(EXPERTS, CAP), live.reshape(EXPERTS, CAP)


def reference(tokens, routing, gate_codes, w_gate, w_up, w_down):
    groups = N_AA * N_COL
    slot, slot_token, live = jax.vmap(slot_tables)(routing.reshape(groups, TOK_DEV, TOP))
    grouped = tokens.reshape(groups, TOK_DEV, D)
    width = FF // N_BA
    group_ids = jnp.arange(groups, dtype=jnp.int32)[:, None]

    def expert(packed):
        wg, wu, wd, index, alive = packed
        rows = grouped[group_ids, index]
        rows = jnp.where(alive[:, :, None], rows, jnp.zeros((), jnp.bfloat16)).reshape(groups * CAP, D)
        total = jnp.zeros((groups * CAP, D), jnp.float32)
        for part in range(N_BA):
            gate = jnp.dot(rows, wg[:, part * width:(part + 1) * width], preferred_element_type=jnp.float32)
            upper = jnp.dot(rows, wu[:, part * width:(part + 1) * width], preferred_element_type=jnp.float32)
            hidden = (jax.nn.silu(gate) * upper).astype(jnp.bfloat16)
            piece = jnp.dot(hidden, wd[part * width:(part + 1) * width, :], preferred_element_type=jnp.float32)
            piece = lax.optimization_barrier(piece.astype(jnp.bfloat16))
            total = total + piece.astype(jnp.float32)
        return total.astype(jnp.bfloat16).reshape(groups, CAP, D)

    outputs = lax.map(expert, (w_gate, w_up, w_down, jnp.transpose(slot_token, (1, 0, 2)), jnp.transpose(live, (1, 0, 2))))
    outputs = jnp.transpose(outputs, (1, 0, 2, 3)).reshape(groups, EXPERTS * CAP, D)
    codes = gate_codes.astype(jnp.float32)
    weight = route_scale * codes / jnp.sum(codes, axis=1, keepdims=True)
    weight = weight.reshape(groups, TOK_DEV, TOP)

    def combine(packed):
        table, slots, scores = packed
        picked = table[slots].reshape(TOK_DEV, TOP, D).astype(jnp.float32)
        return jnp.einsum("tk,tkd->td", scores, picked).astype(jnp.bfloat16)

    mixed = lax.map(combine, (outputs, slot, weight))
    return mixed.reshape(TOKENS, D)
```

```python
import functools
import jax
import jax.numpy as jnp
from jax import lax
from jax.experimental import pallas as pl
from jax.experimental.pallas import tpu as pltpu
from jax.sharding import PartitionSpec as P

MESH = pl.DeviceIdType.MESH
route_scale = 2.827
bf16 = jnp.bfloat16
f32 = jnp.float32
TILE = 128
ORDERS = (("x", "y", "z"), ("y", "z", "x"), ("z", "x", "y"))


def route_tables(routing, experts, slots_each, top):
    flat = routing.reshape(-1)
    onehot = (flat[:, None] == jnp.arange(experts, dtype=jnp.int32)[None, :]).astype(jnp.int32)
    before = jnp.cumsum(onehot, axis=0) - onehot
    pos = jnp.sum(before * onehot, axis=1)
    slot = flat * slots_each + pos
    matched = slot[:, None] == jnp.arange(experts * slots_each, dtype=jnp.int32)[None, :]
    owner = jnp.arange(flat.shape[0], dtype=jnp.int32) // top
    slot_token = jnp.sum(jnp.where(matched, owner[:, None], 0), axis=0)
    live = jnp.any(matched, axis=0)
    return (slot, slot_token.reshape(experts, slots_each), live.reshape(experts, slots_each))


def place():
    aa = lax.axis_index("aa")
    z, core = aa // 2, aa % 2
    return {"z": z, "y": lax.axis_index("ba"), "x": lax.axis_index("col")}, core


def peer(me, core, axis, step):
    at = lax.rem(me[axis] + (step + 4), 4)
    if axis == "z":
        return {"aa": at * 2 + core}
    return {"ba": at} if axis == "y" else {"col": at}


def greet(me, core):
    barrier = pltpu.get_barrier_semaphore()
    for axis in "xyz":
        for step in (1, -1):
            pl.semaphore_signal(barrier, inc=1, device_id=peer(me, core, axis, step), device_id_type=MESH)
    pl.semaphore_signal(barrier, inc=1, device_id={"aa": me["z"] * 2 + (1 - core)}, device_id_type=MESH)
    pl.semaphore_wait(barrier, 7)


def combine_kernel(slots, own_ref, other_ref, down_ref, spread_ref, out_ref,
                   send_rows, pair_rows, in1, in2, in3, got1, got2, got3, more1, more2, more3,
                   send_sem, recv_sem, pair_send, pair_recv, credit):
    me, core = place()
    partner = {"aa": me["z"] * 2 + (1 - core)}
    ins, gots, mores = (in1, in2, in3), (got1, got2, got3), (more1, more2, more3)
    quarter = out_ref.shape[1]
    greet(me, core)

    def ring(r, phase, slot, kind):
        p = lax.rem(slot, 2)
        buf = ins[phase].at[r, p]
        b = ins[phase].shape[2] // 4
        h = b // 2
        axis = ORDERS[r][phase]
        src, dst, step = (
            (buf.at[pl.ds(b + h, b)], gots[phase].at[r, p, 0], 1),
            (buf.at[pl.ds(2 * b + h, b)], gots[phase].at[r, p, 1], -1),
            (buf.at[pl.ds(b, h)], mores[phase].at[r, p, 0], 1),
            (buf.at[pl.ds(3 * b + h, h)], mores[phase].at[r, p, 1], -1),
        )[kind]
        return pltpu.make_async_remote_copy(
            src_ref=src, dst_ref=dst, send_sem=send_sem.at[r, phase, kind, p], recv_sem=recv_sem.at[r, phase, kind, p],
            device_id=peer(me, core, axis, step), device_id_type=MESH)

    def pair(r, slot):
        p = lax.rem(slot, 2)
        return pltpu.make_async_remote_copy(
            src_ref=send_rows.at[r], dst_ref=pair_rows.at[r, p, :, pl.ds(80, 80)], send_sem=pair_send.at[r],
            recv_sem=pair_recv.at[r, p], device_id=partner, device_id_type=MESH)

    def tiles(rows, body):
        size = min(rows, 256)
        if rows == size:
            body(0, size)
        else:
            @pl.loop(0, rows // size)
            def _(i):
                body(pl.multiple_of(i * size, size), size)

    def project(r, slot):
        p = lax.rem(slot, 2)
        first = (slot * 3 + r) * TILE
        w = jnp.concatenate(
            [down_ref[:, pl.ds(pl.multiple_of(q * quarter + first, TILE), TILE)] for q in range(4)], axis=1)
        pair_rows[r, p, :, 0:80, :] = jnp.dot(own_ref[...], w, preferred_element_type=f32).astype(bf16).reshape(8, 80, 4 * TILE)

        @pl.when(slot >= 1)
        def _():
            pair(r, slot - 1).wait_send()

        send_rows[r] = jnp.dot(other_ref[...], w, preferred_element_type=f32).astype(bf16).reshape(8, 80, 4 * TILE)
        pair(r, slot).start()

        @pl.when(slot == slots[r] - 1)
        def _():
            pair(r, slot).wait_send()

    def begin(r, phase, slot):
        @pl.when(slot >= 2)
        def _():
            pl.semaphore_wait(credit.at[r, phase, 0], 1)
            pl.semaphore_wait(credit.at[r, phase, 1], 1)

        ring(r, phase, slot, 0).start()
        ring(r, phase, slot, 1).start()

    def scatter(r, slot):
        p = lax.rem(slot, 2)
        pair(r, slot).wait_recv()
        weight = {axis: 4 ** (2 - ORDERS[r].index(axis)) for axis in "xyz"}

        @pl.loop(0, 8)
        def _(n):
            z = n // 2
            rows = jnp.dot(spread_ref[n], pair_rows[r, p, n], preferred_element_type=f32).astype(bf16)
            to_z = lax.rem(z - me["z"] + 4, 4) * weight["z"]
            for half in range(2):
                x = lax.rem(n, 2) * 2 + half
                to_zx = to_z + lax.rem(x - me["x"] + 4, 4) * weight["x"]
                for q in range(4):
                    at = to_zx + lax.rem(q - me["y"] + 4, 4) * weight["y"]
                    in1[r, p, pl.ds(pl.multiple_of(at * 128, 128), 128), :] = rows[half * 128:half * 128 + 128, q * TILE:(q + 1) * TILE]
        begin(r, 0, slot)

    def middle(r, phase, slot):
        p = lax.rem(slot, 2)
        buf, got = ins[phase], gots[phase]
        b = buf.shape[2] // 4
        h = b // 2
        ring(r, phase, slot, 0).wait_recv()

        def right(i, n):
            a = buf[r, p, pl.ds(b + i, n), :].astype(f32) + got[r, p, 0, pl.ds(h + i, n), :].astype(f32)
            buf[r, p, pl.ds(b + i, n), :] = a.astype(bf16)
        tiles(h, right)
        ring(r, phase, slot, 2).start()
        ring(r, phase, slot, 1).wait_recv()

        def left(i, n):
            a = buf[r, p, pl.ds(3 * b + h + i, n), :].astype(f32) + got[r, p, 1, pl.ds(i, n), :].astype(f32)
            buf[r, p, pl.ds(3 * b + h + i, n), :] = a.astype(bf16)
        tiles(h, left)
        ring(r, phase, slot, 3).start()

    def finish(r, phase, slot):
        p = lax.rem(slot, 2)
        buf, got, more = ins[phase], gots[phase], mores[phase]
        b = buf.shape[2] // 4
        h = b // 2
        ring(r, phase, slot, 2).wait_recv()
        ring(r, phase, slot, 3).wait_recv()

        def put(at, n, value):
            if phase < 2:
                ins[phase + 1][r, p, pl.ds(at, n), :] = value.astype(bf16)
            else:
                col = pl.multiple_of((slot * 3 + r) * TILE, TILE)
                out_ref[pl.ds(at, n), pl.ds(col, TILE)] = value.astype(bf16)

        def first(i, n):
            put(i, n, buf[r, p, pl.ds(i, n), :].astype(f32) + got[r, p, 1, pl.ds(h + i, n), :].astype(f32)
                + more[r, p, 0, pl.ds(i, n), :].astype(f32))
        tiles(h, first)

        def second(i, n):
            put(h + i, n, buf[r, p, pl.ds(h + i, n), :].astype(f32) + got[r, p, 0, pl.ds(i, n), :].astype(f32)
                + more[r, p, 1, pl.ds(i, n), :].astype(f32))
        tiles(h, second)
        for kind in range(4):
            ring(r, phase, slot, kind).wait_send()

        @pl.when(slot + 2 < slots[r])
        def _():
            axis = ORDERS[r][phase]
            pl.semaphore_signal(credit.at[r, phase, 0], inc=1, device_id=peer(me, core, axis, 1), device_id_type=MESH)
            pl.semaphore_signal(credit.at[r, phase, 1], inc=1, device_id=peer(me, core, axis, -1), device_id_type=MESH)

        if phase < 2:
            begin(r, phase + 1, slot)

    def stage(step, delay, body):
        for r in range(3):
            slot = step - delay

            @pl.when((slot >= 0) & (slot < slots[r]))
            def _():
                body(r, slot)

    @pl.loop(0, max(slots) + 7)
    def _(step):
        stage(step, 2, lambda r, s: middle(r, 0, s))
        stage(step, 4, lambda r, s: middle(r, 1, s))
        stage(step, 6, lambda r, s: middle(r, 2, s))
        stage(step, 7, lambda r, s: finish(r, 2, s))
        stage(step, 5, lambda r, s: finish(r, 1, s))
        stage(step, 3, lambda r, s: finish(r, 0, s))
        stage(step, 1, scatter)
        stage(step, 0, project)


def combine(own, other, down, spread):
    quarter = down.shape[1] // 4
    count = quarter // TILE
    slots = tuple((count - r + 2) // 3 for r in range(3))
    vmem = pl.BlockSpec(memory_space=pltpu.VMEM)

    def buffers(parts, rows):
        return pltpu.VMEM((3, 2) + parts + (rows, TILE), bf16)

    return pl.pallas_call(
        functools.partial(combine_kernel, slots),
        out_shape=jax.ShapeDtypeStruct((128, quarter), bf16),
        in_specs=[vmem] * 4,
        out_specs=vmem,
        scratch_shapes=[
            pltpu.VMEM((3, 8, 80, 4 * TILE), bf16),
            pltpu.VMEM((3, 2, 8, 160, 4 * TILE), bf16),
            buffers((), 8192), buffers((), 2048), buffers((), 512),
            buffers((2,), 2048), buffers((2,), 512), buffers((2,), 128),
            buffers((2,), 1024), buffers((2,), 256), buffers((2,), 64),
            pltpu.SemaphoreType.DMA((3, 3, 4, 2)),
            pltpu.SemaphoreType.DMA((3, 3, 4, 2)),
            pltpu.SemaphoreType.DMA((3,)),
            pltpu.SemaphoreType.DMA((3, 2)),
            pltpu.SemaphoreType.REGULAR((3, 3, 2)),
        ],
        compiler_params=pltpu.CompilerParams(collective_id=1, has_side_effects=True, vmem_limit_bytes=66000000),
        name="combine",
    )(own, other, down, spread)


def expert_tables(routing, weight, expert, cap):
    named = routing == expert
    taken = jnp.any(named, axis=2)
    ones = taken.astype(f32)
    rank = jnp.arange(128)
    pos = jnp.dot(ones, (rank[:, None] < rank[None, :]).astype(f32)).astype(jnp.int32)
    hot = taken[:, :, None] & (pos[:, :, None] == jnp.arange(cap, dtype=jnp.int32)[None, None, :])
    gain = jnp.sum(jnp.where(named, weight, 0.0), axis=2)
    return hot, jnp.sum(jnp.where(hot, gain[:, :, None], 0.0), axis=1)


def spread_matrix(hot_own, hot_other, core):
    def mine(hot):
        by = hot.reshape(4, 2, 2, 2, 128, 40)
        return lax.dynamic_index_in_dim(by, core, 1, keepdims=False)
    both = jnp.stack([mine(hot_own), mine(hot_other)], axis=4)
    eye = jnp.eye(2, dtype=bool)
    wide = both[:, :, :, :, :, None, :] & eye[None, None, :, None, None, :, None]
    return wide.reshape(8, 256, 160).astype(bf16)


def on_device(tokens, routing, gate_codes, w_gate, w_up, w_down):
    experts = lax.axis_size("aa") * lax.axis_size("col")
    tok_rows = tokens.shape[0]
    top = routing.shape[1]
    cap = min(tok_rows, 5 * tok_rows * top // (4 * experts))
    aa, col = lax.axis_index("aa"), lax.axis_index("col")
    core = aa % 2
    slot, slot_token, live = route_tables(routing, experts, cap, top)
    all_codes = lax.all_gather(jnp.concatenate([routing, gate_codes], axis=1), ("aa", "col"), axis=0, tiled=False)
    all_routing = all_codes[:, :, :top]
    codes = all_codes[:, :, top:].astype(f32)
    weight = route_scale * codes / jnp.sum(codes, axis=2, keepdims=True)
    hot_own, gain_own = expert_tables(all_routing, weight, aa * 4 + col, cap)
    hot_other, _ = expert_tables(all_routing, weight, (aa + 1 - 2 * core) * 4 + col, cap)
    spread = spread_matrix(hot_own, hot_other, core)
    outgoing = jnp.where(live[:, :, None], tokens[slot_token], jnp.zeros((), bf16))
    full_rows = lax.all_gather(
        lax.all_to_all(outgoing, ("aa", "col"), split_axis=0, concat_axis=0, tiled=True),
        "ba",
        axis=2,
        tiled=True,
    )
    rows = full_rows.reshape(experts * cap, full_rows.shape[2])
    gate = jnp.dot(rows, w_gate[0], preferred_element_type=f32)
    upper = jnp.dot(rows, w_up[0], preferred_element_type=f32)
    hidden = (jax.nn.silu(gate) * upper * gain_own.reshape(-1, 1)).astype(bf16)
    by_core = hidden.reshape(4, 2, 160, hidden.shape[1])
    own = lax.dynamic_index_in_dim(by_core, core, 1, keepdims=False).reshape(640, -1)
    other = lax.dynamic_index_in_dim(by_core, 1 - core, 1, keepdims=False).reshape(640, -1)
    return combine(own, other, w_down[0], spread)


def solution(mesh):
    return jax.shard_map(
        on_device,
        mesh=mesh,
        in_specs=(
            P(("aa", "col"), "ba"),
            P(("aa", "col"), None),
            P(("aa", "col"), None),
            P(("aa", "col"), None, "ba"),
            P(("aa", "col"), None, "ba"),
            P(("aa", "col"), "ba", None),
        ),
        out_specs=P(("aa", "col"), "ba"),
        check_vma=False,
    )
```

```python
import functools
import jax
import jax.numpy as jnp
from jax import lax
from jax.experimental import pallas as pl
from jax.experimental.pallas import tpu as pltpu
from jax.sharding import PartitionSpec as P

MESH = pl.DeviceIdType.MESH
route_scale = 2.827
bf16 = jnp.bfloat16
f32 = jnp.float32
TILE = 128
ORDERS = (("x", "y", "z"), ("y", "z", "x"), ("z", "x", "y"))


def place():
    aa = lax.axis_index("aa")
    z, core = aa // 2, aa % 2
    return {"z": z, "y": lax.axis_index("ba"), "x": lax.axis_index("col")}, core


def peer(me, core, axis, step):
    at = lax.rem(me[axis] + (step + 4), 4)
    if axis == "z":
        return {"aa": at * 2 + core}
    return {"ba": at} if axis == "y" else {"col": at}


def greet(me, core):
    barrier = pltpu.get_barrier_semaphore()
    for axis in "xyz":
        for step in (1, -1):
            pl.semaphore_signal(barrier, inc=1, device_id=peer(me, core, axis, step), device_id_type=MESH)
    pl.semaphore_signal(barrier, inc=1, device_id={"aa": me["z"] * 2 + (1 - core)}, device_id_type=MESH)
    pl.semaphore_wait(barrier, 7)


def pick_tables(core_groups, experts, put_pick, put_gain):
    lane = lax.broadcasted_iota(jnp.int32, (128, 128), 1)
    row = lax.broadcasted_iota(jnp.int32, (128, 128), 0)
    before = (row < lane).astype(bf16)
    slot_row = lax.broadcasted_iota(jnp.int32, (80, 256), 0)
    half_lane = lax.broadcasted_iota(jnp.int32, (80, 256), 1)
    second_row, second_lane = slot_row >= 40, half_lane >= 128
    position = jnp.where(second_row, slot_row - 40, slot_row).astype(f32)
    same = second_row == second_lane
    for source, expert in enumerate(experts):
        taken, pos, gain = [], [], []
        for block in core_groups:
            block = block.astype(f32)
            code = block[8:16] * 256.0 + block[16:24]
            weight = route_scale * code / jnp.sum(code, axis=0, keepdims=True)
            named = block[0:8] == expert
            hit = jnp.max(jnp.where(named, 1.0, 0.0), axis=0, keepdims=True)
            taken.append(hit)
            wide = jnp.broadcast_to(hit, (8, 128)).astype(bf16)
            pos.append(jnp.dot(wide, before, preferred_element_type=f32)[0:1])
            gain.append(jnp.sum(jnp.where(named, weight, 0.0), axis=0, keepdims=True))
        taken, pos, gain = (jnp.concatenate(v, axis=1) for v in (taken, pos, gain))
        hot = same & (pos == position) & (taken > 0.5)
        put_pick(source, jnp.where(hot, 1.0, 0.0).astype(bf16))
        put_gain(source, jnp.broadcast_to(jnp.sum(jnp.where(hot, gain, 0.0), axis=1, keepdims=True), (80, 128)))


def dispatch_kernel(slots, tok_ref, meta_ref, gate_hbm, up_hbm, own_ref, other_ref, pick_ref,
                    gate_ref, up_ref, total, out1, out2, out3, rows_own, rows_send, rows_got, gain_own, gain_send, gain_got,
                    send_sem, recv_sem, pair_send, pair_recv, gain_sem, load_sem, credit):
    me, core = place()
    partner = {"aa": me["z"] * 2 + (1 - core)}
    outs = (out1, out2, out3)
    quarter = tok_ref.shape[1]
    loads = [pltpu.make_async_copy(gate_hbm, gate_ref, load_sem.at[0]), pltpu.make_async_copy(up_hbm, up_ref, load_sem.at[1])]
    for load in loads:
        load.start()
    greet(me, core)

    def tile_of(r, slot):
        return pl.multiple_of((slot * 3 + (r + 1) % 3 - 1) * TILE, TILE)

    def ring(r, phase, slot, kind):
        p = lax.rem(slot, outs[phase].shape[1])
        buf = outs[phase].at[r, p]
        b = outs[phase].shape[2] // 4
        h = b // 2
        axis = ORDERS[r][phase]
        src, dst, step = (
            (pl.ds(0, b), pl.ds(3 * b, b), 1),
            (pl.ds(0, b), pl.ds(b, b), -1),
            (pl.ds(3 * b, h), pl.ds(2 * b, h), 1),
            (pl.ds(b + h, h), pl.ds(2 * b + h, h), -1),
        )[kind]
        return pltpu.make_async_remote_copy(
            src_ref=buf.at[src], dst_ref=buf.at[dst], send_sem=send_sem.at[r, phase, kind, p],
            recv_sem=recv_sem.at[r, phase, kind, p], device_id=peer(me, core, axis, step), device_id_type=MESH)

    def pair(r, slot):
        p = lax.rem(slot, 2)
        return pltpu.make_async_remote_copy(
            src_ref=rows_send.at[r], dst_ref=rows_got.at[r, p], send_sem=pair_send.at[r], recv_sem=pair_recv.at[r, p],
            device_id=partner, device_id_type=MESH)

    gains = pltpu.make_async_remote_copy(
        src_ref=gain_send, dst_ref=gain_got, send_sem=gain_sem.at[0], recv_sem=gain_sem.at[1],
        device_id=partner, device_id_type=MESH)

    def begin(r, phase, slot):
        @pl.when(slot >= outs[phase].shape[1])
        def _():
            pl.semaphore_wait(credit.at[r, phase, 0], 1)
            pl.semaphore_wait(credit.at[r, phase, 1], 1)

        ring(r, phase, slot, 0).start()
        ring(r, phase, slot, 1).start()

    def open_tile(r, slot):
        p = lax.rem(slot, 2)

        def tokens():
            out1[r, p, 0:128, :] = tok_ref[:, pl.ds(tile_of(r, slot), TILE)]

        if r == 2:
            @pl.when(slot == 0)
            def _():
                out1[r, p, 0:128, :] = meta_ref[...]

            pl.when(slot > 0)(tokens)
        else:
            tokens()
        begin(r, 0, slot)

    def middle(r, phase, slot):
        ring(r, phase, slot, 0).wait_recv()
        ring(r, phase, slot, 2).start()
        ring(r, phase, slot, 1).wait_recv()
        ring(r, phase, slot, 3).start()

    def close(r, phase, slot):
        for kind in range(4):
            ring(r, phase, slot, kind).wait_send()

        @pl.when(slot + outs[phase].shape[1] < slots[r])
        def _():
            axis = ORDERS[r][phase]
            pl.semaphore_signal(credit.at[r, phase, 0], inc=1, device_id=peer(me, core, axis, 1), device_id_type=MESH)
            pl.semaphore_signal(credit.at[r, phase, 1], inc=1, device_id=peer(me, core, axis, -1), device_id_type=MESH)

    def finish(r, phase, slot):
        ring(r, phase, slot, 2).wait_recv()
        ring(r, phase, slot, 3).wait_recv()
        src, dst = outs[phase], outs[phase + 1]
        p, q = lax.rem(slot, src.shape[1]), lax.rem(slot, dst.shape[1])

        @pl.loop(0, src.shape[2] // 512)
        def _(i):
            at = pl.multiple_of(i * 512, 512)
            dst[r, q, pl.ds(at, 512), :] = src[r, p, pl.ds(at, 512), :]
        begin(r, phase + 1, slot)
        close(r, phase, slot)

    def block_of(r, z, x, y):
        weight = {axis: 4 ** ORDERS[r].index(axis) for axis in "xyz"}
        at = sum(lax.rem(there - me[axis] + 4, 4) * weight[axis] for axis, there in (("z", z), ("x", x), ("y", y)))
        return pl.multiple_of(at * 128, 128)

    def tables(r, slot):
        experts = [(((me["z"] * 2 + c) * 4) + me["x"]).astype(f32) for c in (core, 1 - core)]

        @pl.loop(0, 8)
        def _(n):
            z = n // 2
            blocks = [out3[r, 0, pl.ds(block_of(r, z, lax.rem(n, 2) * 2 + half, me["y"]), 32), :] for half in range(2)]

            def put_pick(source, hot):
                pick_ref[n, source * 80:source * 80 + 80, :] = hot

            def put_gain(source, gain):
                (gain_own, gain_send)[source][n] = gain
            pick_tables(blocks, experts, put_pick, put_gain)
        gains.start()

    def select(r, slot):
        p = lax.rem(slot, out3.shape[1])

        @pl.when(slot >= (2 if r == 2 else 1))
        def _():
            pair(r, slot - 1).wait_send()

        @pl.loop(0, 8)
        def _(n):
            z = n // 2
            wide = [jnp.concatenate([out3[r, p, pl.ds(block_of(r, z, lax.rem(n, 2) * 2 + half, q), 128), :] for q in range(4)], axis=1)
                    for half in range(2)]
            rows = jnp.dot(pick_ref[n], jnp.concatenate(wide, axis=0), preferred_element_type=f32).astype(bf16)
            at = pl.ds(pl.multiple_of(n * 80, 16), 80)
            rows_own[r, at, :] = rows[0:80]
            rows_send[r, at, :] = rows[80:160]
        pair(r, slot).start()

        @pl.when(slot == slots[r] - 1)
        def _():
            pair(r, slot).wait_send()

    def gather(r, slot):
        ring(r, 2, slot, 2).wait_recv()
        ring(r, 2, slot, 3).wait_recv()
        if r == 2:
            pl.when(slot == 0)(lambda: tables(r, slot))
            pl.when(slot > 0)(lambda: select(r, slot))
        else:
            select(r, slot)
        close(r, 2, slot)

    def multiply(r, slot):
        p = lax.rem(slot, 2)

        def work():
            pair(r, slot).wait_recv()
            first = tile_of(r, slot)
            for w_ref, col in ((gate_ref, 0), (up_ref, 512)):
                w = jnp.concatenate([w_ref[pl.ds(pl.multiple_of(q * quarter + first, TILE), TILE), :] for q in range(4)], axis=0)
                total[0, :, col:col + 512] += jnp.dot(rows_own[r], w, preferred_element_type=f32)
                total[1, :, col:col + 512] += jnp.dot(rows_got[r, p], w, preferred_element_type=f32)

        if r == 2:
            pl.when(slot > 0)(work)
        else:
            work()

    def stage(step, delay, body):
        for r in (2, 0, 1):
            slot = step - delay

            @pl.when((slot >= 0) & (slot < slots[r]))
            def _():
                body(r, slot)

    @pl.loop(0, max(slots) + 6)
    def _(step):
        stage(step, 5, lambda r, s: middle(r, 2, s))
        stage(step, 4, lambda r, s: finish(r, 1, s))
        stage(step, 3, lambda r, s: middle(r, 1, s))
        stage(step, 2, lambda r, s: finish(r, 0, s))
        stage(step, 1, lambda r, s: middle(r, 0, s))
        stage(step, 0, open_tile)
        stage(step, 6, gather)

        @pl.when(step == 6)
        def _():
            total[...] = jnp.zeros_like(total)
            for load in loads:
                load.wait()

        stage(step, 6, multiply)

    gains.wait()

    @pl.loop(0, 8)
    def _(n):
        at = pl.ds(pl.multiple_of(n * 80, 16), 80)
        for half, ref, gain in ((0, own_ref, gain_own), (1, other_ref, gain_got)):
            gate = total[half, at, 0:512]
            upper = total[half, at, 512:1024]
            ref[at, :] = (jax.nn.silu(gate) * upper * gain[n][:, 0:1]).astype(bf16)


def dispatch(tokens, meta, gate, up):
    quarter = tokens.shape[1]
    count = quarter // TILE + 1
    slots = tuple((count - (r + 1) % 3 + 2) // 3 for r in range(3))
    vmem = pl.BlockSpec(memory_space=pltpu.VMEM)
    hbm = pl.BlockSpec(memory_space=pl.ANY)
    hidden = jax.ShapeDtypeStruct((640, 512), bf16)
    return pl.pallas_call(
        functools.partial(dispatch_kernel, slots),
        out_shape=(hidden, hidden, jax.ShapeDtypeStruct((8, 160, 256), bf16)),
        in_specs=[vmem, vmem, hbm, hbm],
        out_specs=(vmem,) * 3,
        scratch_shapes=[
            pltpu.VMEM(gate.shape, bf16), pltpu.VMEM(up.shape, bf16), pltpu.VMEM((2, 640, 1024), f32),
            pltpu.VMEM((3, 2, 512, TILE), bf16), pltpu.VMEM((3, 2, 2048, TILE), bf16), pltpu.VMEM((3, 3, 8192, TILE), bf16),
            pltpu.VMEM((3, 640, 4 * TILE), bf16), pltpu.VMEM((3, 640, 4 * TILE), bf16), pltpu.VMEM((3, 2, 640, 4 * TILE), bf16),
            pltpu.VMEM((8, 80, 128), f32), pltpu.VMEM((8, 80, 128), f32), pltpu.VMEM((8, 80, 128), f32),
            pltpu.SemaphoreType.DMA((3, 3, 4, 3)),
            pltpu.SemaphoreType.DMA((3, 3, 4, 3)),
            pltpu.SemaphoreType.DMA((3,)),
            pltpu.SemaphoreType.DMA((3, 2)),
            pltpu.SemaphoreType.DMA((2,)),
            pltpu.SemaphoreType.DMA((2,)),
            pltpu.SemaphoreType.REGULAR((3, 3, 2)),
        ],
        compiler_params=pltpu.CompilerParams(collective_id=0, has_side_effects=True, vmem_limit_bytes=66000000),
        name="dispatch",
    )(tokens, meta, gate, up)


def combine_kernel(slots, own_ref, other_ref, down_ref, pick_ref, out_ref,
                   send_rows, pair_rows, in1, in2, in3, got1, got2, got3, more1, more2, more3,
                   send_sem, recv_sem, pair_send, pair_recv, credit):
    me, core = place()
    partner = {"aa": me["z"] * 2 + (1 - core)}
    ins, gots, mores = (in1, in2, in3), (got1, got2, got3), (more1, more2, more3)
    quarter = out_ref.shape[1]
    greet(me, core)

    def ring(r, phase, slot, kind):
        p = lax.rem(slot, 2)
        buf = ins[phase].at[r, p]
        b = ins[phase].shape[2] // 4
        h = b // 2
        axis = ORDERS[r][phase]
        src, dst, step = (
            (buf.at[pl.ds(b + h, b)], gots[phase].at[r, p, 0], 1),
            (buf.at[pl.ds(2 * b + h, b)], gots[phase].at[r, p, 1], -1),
            (buf.at[pl.ds(b, h)], mores[phase].at[r, p, 0], 1),
            (buf.at[pl.ds(3 * b + h, h)], mores[phase].at[r, p, 1], -1),
        )[kind]
        return pltpu.make_async_remote_copy(
            src_ref=src, dst_ref=dst, send_sem=send_sem.at[r, phase, kind, p], recv_sem=recv_sem.at[r, phase, kind, p],
            device_id=peer(me, core, axis, step), device_id_type=MESH)

    def pair(r, slot):
        p = lax.rem(slot, 2)
        return pltpu.make_async_remote_copy(
            src_ref=send_rows.at[r], dst_ref=pair_rows.at[r, p, :, pl.ds(80, 80)], send_sem=pair_send.at[r],
            recv_sem=pair_recv.at[r, p], device_id=partner, device_id_type=MESH)

    def tiles(rows, body):
        size = min(rows, 256)
        if rows == size:
            body(0, size)
        else:
            @pl.loop(0, rows // size)
            def _(i):
                body(pl.multiple_of(i * size, size), size)

    def project(r, slot):
        p = lax.rem(slot, 2)
        first = (slot * 3 + r) * TILE
        w = jnp.concatenate(
            [down_ref[:, pl.ds(pl.multiple_of(q * quarter + first, TILE), TILE)] for q in range(4)], axis=1)
        pair_rows[r, p, :, 0:80, :] = jnp.dot(own_ref[...], w, preferred_element_type=f32).astype(bf16).reshape(8, 80, 4 * TILE)

        @pl.when(slot >= 1)
        def _():
            pair(r, slot - 1).wait_send()

        send_rows[r] = jnp.dot(other_ref[...], w, preferred_element_type=f32).astype(bf16).reshape(8, 80, 4 * TILE)
        pair(r, slot).start()

        @pl.when(slot == slots[r] - 1)
        def _():
            pair(r, slot).wait_send()

    def begin(r, phase, slot):
        @pl.when(slot >= 2)
        def _():
            pl.semaphore_wait(credit.at[r, phase, 0], 1)
            pl.semaphore_wait(credit.at[r, phase, 1], 1)

        ring(r, phase, slot, 0).start()
        ring(r, phase, slot, 1).start()

    def scatter(r, slot):
        p = lax.rem(slot, 2)
        pair(r, slot).wait_recv()
        weight = {axis: 4 ** (2 - ORDERS[r].index(axis)) for axis in "xyz"}

        @pl.loop(0, 8)
        def _(n):
            z = n // 2
            rows = lax.dot_general(pick_ref[n], pair_rows[r, p, n], (((0,), (0,)), ((), ())), preferred_element_type=f32).astype(bf16)
            to_z = lax.rem(z - me["z"] + 4, 4) * weight["z"]
            for half in range(2):
                x = lax.rem(n, 2) * 2 + half
                to_zx = to_z + lax.rem(x - me["x"] + 4, 4) * weight["x"]
                for q in range(4):
                    at = to_zx + lax.rem(q - me["y"] + 4, 4) * weight["y"]
                    in1[r, p, pl.ds(pl.multiple_of(at * 128, 128), 128), :] = rows[half * 128:half * 128 + 128, q * TILE:(q + 1) * TILE]
        begin(r, 0, slot)

    def middle(r, phase, slot):
        p = lax.rem(slot, 2)
        buf, got = ins[phase], gots[phase]
        b = buf.shape[2] // 4
        h = b // 2
        ring(r, phase, slot, 0).wait_recv()

        def right(i, n):
            a = buf[r, p, pl.ds(b + i, n), :].astype(f32) + got[r, p, 0, pl.ds(h + i, n), :].astype(f32)
            buf[r, p, pl.ds(b + i, n), :] = a.astype(bf16)
        tiles(h, right)
        ring(r, phase, slot, 2).start()
        ring(r, phase, slot, 1).wait_recv()

        def left(i, n):
            a = buf[r, p, pl.ds(3 * b + h + i, n), :].astype(f32) + got[r, p, 1, pl.ds(i, n), :].astype(f32)
            buf[r, p, pl.ds(3 * b + h + i, n), :] = a.astype(bf16)
        tiles(h, left)
        ring(r, phase, slot, 3).start()

    def finish(r, phase, slot):
        p = lax.rem(slot, 2)
        buf, got, more = ins[phase], gots[phase], mores[phase]
        b = buf.shape[2] // 4
        h = b // 2
        ring(r, phase, slot, 2).wait_recv()
        ring(r, phase, slot, 3).wait_recv()

        def put(at, n, value):
            if phase < 2:
                ins[phase + 1][r, p, pl.ds(at, n), :] = value.astype(bf16)
            else:
                col = pl.multiple_of((slot * 3 + r) * TILE, TILE)
                out_ref[pl.ds(at, n), pl.ds(col, TILE)] = value.astype(bf16)

        def first(i, n):
            put(i, n, buf[r, p, pl.ds(i, n), :].astype(f32) + got[r, p, 1, pl.ds(h + i, n), :].astype(f32)
                + more[r, p, 0, pl.ds(i, n), :].astype(f32))
        tiles(h, first)

        def second(i, n):
            put(h + i, n, buf[r, p, pl.ds(h + i, n), :].astype(f32) + got[r, p, 0, pl.ds(i, n), :].astype(f32)
                + more[r, p, 1, pl.ds(i, n), :].astype(f32))
        tiles(h, second)
        for kind in range(4):
            ring(r, phase, slot, kind).wait_send()

        @pl.when(slot + 2 < slots[r])
        def _():
            axis = ORDERS[r][phase]
            pl.semaphore_signal(credit.at[r, phase, 0], inc=1, device_id=peer(me, core, axis, 1), device_id_type=MESH)
            pl.semaphore_signal(credit.at[r, phase, 1], inc=1, device_id=peer(me, core, axis, -1), device_id_type=MESH)

        if phase < 2:
            begin(r, phase + 1, slot)

    def stage(step, delay, body):
        for r in range(3):
            slot = step - delay

            @pl.when((slot >= 0) & (slot < slots[r]))
            def _():
                body(r, slot)

    @pl.loop(0, max(slots) + 7)
    def _(step):
        stage(step, 2, lambda r, s: middle(r, 0, s))
        stage(step, 4, lambda r, s: middle(r, 1, s))
        stage(step, 6, lambda r, s: middle(r, 2, s))
        stage(step, 7, lambda r, s: finish(r, 2, s))
        stage(step, 5, lambda r, s: finish(r, 1, s))
        stage(step, 3, lambda r, s: finish(r, 0, s))
        stage(step, 1, scatter)
        stage(step, 0, project)


def combine(own, other, down, pick):
    quarter = down.shape[1] // 4
    count = quarter // TILE
    slots = tuple((count - r + 2) // 3 for r in range(3))
    vmem = pl.BlockSpec(memory_space=pltpu.VMEM)

    def buffers(parts, rows):
        return pltpu.VMEM((3, 2) + parts + (rows, TILE), bf16)

    return pl.pallas_call(
        functools.partial(combine_kernel, slots),
        out_shape=jax.ShapeDtypeStruct((128, quarter), bf16),
        in_specs=[vmem] * 4,
        out_specs=vmem,
        scratch_shapes=[
            pltpu.VMEM((3, 8, 80, 4 * TILE), bf16),
            pltpu.VMEM((3, 2, 8, 160, 4 * TILE), bf16),
            buffers((), 8192), buffers((), 2048), buffers((), 512),
            buffers((2,), 2048), buffers((2,), 512), buffers((2,), 128),
            buffers((2,), 1024), buffers((2,), 256), buffers((2,), 64),
            pltpu.SemaphoreType.DMA((3, 3, 4, 2)),
            pltpu.SemaphoreType.DMA((3, 3, 4, 2)),
            pltpu.SemaphoreType.DMA((3,)),
            pltpu.SemaphoreType.DMA((3, 2)),
            pltpu.SemaphoreType.REGULAR((3, 3, 2)),
        ],
        compiler_params=pltpu.CompilerParams(collective_id=1, has_side_effects=True, vmem_limit_bytes=66000000),
        name="combine",
    )(own, other, down, pick)


def on_device(tokens, routing, gate_codes, w_gate, w_up, w_down):
    codes = jnp.concatenate([routing, gate_codes // 256, gate_codes % 256], axis=1).astype(bf16).T
    meta = jnp.pad(codes, ((0, 128 - codes.shape[0]), (0, 0)))
    own, other, pick = dispatch(tokens, meta, w_gate[0], w_up[0])
    return combine(own, other, w_down[0], pick)


def solution(mesh):
    return jax.shard_map(
        on_device,
        mesh=mesh,
        in_specs=(
            P(("aa", "col"), "ba"),
            P(("aa", "col"), None),
            P(("aa", "col"), None),
            P(("aa", "col"), None, "ba"),
            P(("aa", "col"), None, "ba"),
            P(("aa", "col"), "ba", None),
        ),
        out_specs=P(("aa", "col"), "ba"),
        check_vma=False,
    )
```

```python
import functools
import jax
import jax.numpy as jnp
from jax import lax
from jax.experimental import pallas as pl
from jax.experimental.pallas import tpu as pltpu
from jax.sharding import PartitionSpec as P

MESH = pl.DeviceIdType.MESH
route_scale = 2.827
bf16 = jnp.bfloat16
f32 = jnp.float32
TILE = 128
STREAMS = ((("z", "x", "y"), 0, 4), (("x", "z", "y"), 4, 4), (("y", "z", "x"), 8, 3), (("y", "x", "z"), 11, 3))
PACKED = 2
RIGHT, LEFT = 1, -1


def place():
    aa = lax.axis_index("aa")
    return {"z": aa // 2, "y": lax.axis_index("ba"), "x": lax.axis_index("col")}, aa % 2


def peer(me, core, axis, step):
    at = lax.rem(me[axis] + (step + 4), 4)
    if axis == "z":
        return {"aa": at * 2 + core}
    return {"ba": at} if axis == "y" else {"col": at}


def greet(me, core):
    barrier = pltpu.get_barrier_semaphore()
    for axis in "xyz":
        for step in (RIGHT, LEFT):
            pl.semaphore_signal(barrier, inc=1, device_id=peer(me, core, axis, step), device_id_type=MESH)
    pl.semaphore_signal(barrier, inc=1, device_id={"aa": me["z"] * 2 + (1 - core)}, device_id_type=MESH)
    pl.semaphore_wait(barrier, 7)


def grant(me, core, credit, phase, axis):
    pl.semaphore_signal(credit.at[phase, 0], inc=1, device_id=peer(me, core, axis, RIGHT), device_id_type=MESH)
    pl.semaphore_signal(credit.at[phase, 1], inc=1, device_id=peer(me, core, axis, LEFT), device_id_type=MESH)


def spend(credit, phase):
    pl.semaphore_wait(credit.at[phase, 0], 1)
    pl.semaphore_wait(credit.at[phase, 1], 1)


def tiles(rows, body):
    size = min(rows, 128 if rows % 256 else 256)
    if rows == size:
        body(0, size)
    else:
        @pl.loop(0, rows // size)
        def _(i):
            body(pl.multiple_of(i * size, size), size)


def block_at(me, weights, there):
    at = sum(lax.rem(spot - me[axis] + 4, 4) * weights[axis] for axis, spot in there.items())
    return pl.multiple_of(at * 128, 128)


def pick_tables(blocks, experts, put_pick, put_gain):
    lane = lax.broadcasted_iota(jnp.int32, (128, 128), 1)
    row = lax.broadcasted_iota(jnp.int32, (128, 128), 0)
    before = (row < lane).astype(bf16)
    slot_row = lax.broadcasted_iota(jnp.int32, (80, 256), 0)
    half_lane = lax.broadcasted_iota(jnp.int32, (80, 256), 1)
    second_row, second_lane = slot_row >= 40, half_lane >= 128
    position = jnp.where(second_row, slot_row - 40, slot_row).astype(f32)
    same = second_row == second_lane
    for source, expert in enumerate(experts):
        taken, pos, gain = [], [], []
        for block in blocks:
            block = block.astype(f32)
            code = block[8:16] * 256.0 + block[16:24]
            weight = route_scale * code / jnp.sum(code, axis=0, keepdims=True)
            named = block[0:8] == expert
            hit = jnp.max(jnp.where(named, 1.0, 0.0), axis=0, keepdims=True)
            taken.append(hit)
            wide = jnp.broadcast_to(hit, (8, 128)).astype(bf16)
            pos.append(jnp.dot(wide, before, preferred_element_type=f32)[0:1])
            gain.append(jnp.sum(jnp.where(named, weight, 0.0), axis=0, keepdims=True))
        taken, pos, gain = (jnp.concatenate(v, axis=1) for v in (taken, pos, gain))
        hot = same & (pos == position) & (taken > 0.5)
        put_pick(source, jnp.where(hot, 1.0, 0.0).astype(bf16))
        put_gain(source, jnp.broadcast_to(jnp.sum(jnp.where(hot, gain, 0.0), axis=1, keepdims=True), (80, 128)))


class Gather:
    def __init__(self, me, core, axes, outs, sends, recvs, credit, slots):
        self.me, self.core, self.axes, self.outs = me, core, axes, outs
        self.sends, self.recvs, self.credit, self.slots = sends, recvs, credit, slots

    def depth(self, phase):
        return self.outs[phase].shape[0]

    def copy(self, phase, slot, kind):
        p = lax.rem(slot, self.depth(phase))
        buf = self.outs[phase].at[p]
        b = self.outs[phase].shape[1] // 4
        h = b // 2
        src, dst, step = (
            (pl.ds(0, b), pl.ds(3 * b, b), RIGHT),
            (pl.ds(0, b), pl.ds(b, b), LEFT),
            (pl.ds(3 * b, h), pl.ds(2 * b, h), RIGHT),
            (pl.ds(b + h, h), pl.ds(2 * b + h, h), LEFT),
        )[kind]
        return pltpu.make_async_remote_copy(
            src_ref=buf.at[src], dst_ref=buf.at[dst], send_sem=self.sends[phase].at[kind, p], recv_sem=self.recvs[phase].at[kind, p],
            device_id=peer(self.me, self.core, self.axes[phase], step), device_id_type=MESH)

    def begin(self, phase, slot):
        if self.slots > self.depth(phase):
            pl.when(slot >= self.depth(phase))(lambda: spend(self.credit, phase))
        self.copy(phase, slot, 0).start()
        self.copy(phase, slot, 1).start()

    def middle(self, phase, slot):
        self.copy(phase, slot, 0).wait_recv()
        self.copy(phase, slot, 2).start()
        self.copy(phase, slot, 1).wait_recv()
        self.copy(phase, slot, 3).start()

    def arrive(self, phase, slot):
        self.copy(phase, slot, 2).wait_recv()
        self.copy(phase, slot, 3).wait_recv()

    def close(self, phase, slot):
        for kind in range(4):
            self.copy(phase, slot, kind).wait_send()
        if self.slots > self.depth(phase):
            pl.when(slot + self.depth(phase) < self.slots)(
                lambda: grant(self.me, self.core, self.credit, phase, self.axes[phase]))

    def forward(self, phase, slot):
        src, dst = self.outs[phase], self.outs[phase + 1]
        p, q = lax.rem(slot, src.shape[0]), lax.rem(slot, dst.shape[0])

        def move(at, n):
            dst[q, pl.ds(at, n), :] = src[p, pl.ds(at, n), :]
        tiles(src.shape[1], move)


def dispatch_kernel(tok_ref, meta_ref, gate_hbm, up_hbm, own_ref, other_ref, pick_ref,
                    gate_ref, up_ref, total, gain_own, gain_send, gain_got, gain_sem, load_sem, credit, *rest):
    rest = list(rest)

    def take(n):
        taken = rest[:n]
        del rest[:n]
        return taken

    me, core = place()
    partner = {"aa": me["z"] * 2 + (1 - core)}
    quarter = tok_ref.shape[1]
    loads = [pltpu.make_async_copy(gate_hbm, gate_ref, load_sem.at[0]), pltpu.make_async_copy(up_hbm, up_ref, load_sem.at[1])]
    for load in loads:
        load.start()
    greet(me, core)
    rings, wares = [], []
    for s, (axes, _, slots) in enumerate(STREAMS):
        rings.append(Gather(me, core, axes, take(3), take(3), take(3), credit.at[s], slots))
        wares.append(take(3 if s < PACKED else 5))
    notes = Gather(me, core, ("x", "z"), take(2), take(2), take(2), None, 1)
    gains = pltpu.make_async_remote_copy(
        src_ref=gain_send, dst_ref=gain_got, send_sem=gain_sem.at[0], recv_sem=gain_sem.at[1],
        device_id=partner, device_id_type=MESH)

    def pair(s, slot, part=0):
        if s < PACKED:
            got, send, recv = wares[s]
            b = got.shape[2]
            src = rings[s].outs[2].at[lax.rem(slot, rings[s].depth(2)), pl.ds(2 * b * part + b, b)]
            dst = got.at[lax.rem(slot, 2), part]
            send_at, recv_at = send.at[part], recv.at[lax.rem(slot, 2), part]
        else:
            _, src, got, send, recv = wares[s]
            dst = got.at[lax.rem(slot, 2)]
            send_at, recv_at = send.at[0], recv.at[lax.rem(slot, 2)]
        return pltpu.make_async_remote_copy(
            src_ref=src, dst_ref=dst, send_sem=send_at, recv_sem=recv_at, device_id=partner, device_id_type=MESH)

    def tile_of(s, slot):
        return pl.multiple_of((slot + STREAMS[s][1]) * TILE, TILE)

    def open_tile(s, slot):
        rings[s].outs[0][lax.rem(slot, 2), 0:128, :] = tok_ref[:, pl.ds(tile_of(s, slot), TILE)]
        rings[s].begin(0, slot)

    def pick(n, blocks):
        return jnp.dot(pick_ref[n], jnp.concatenate(blocks, axis=0), preferred_element_type=f32).astype(bf16)

    def pass_on(s, phase, slot):
        ring = rings[s]
        ring.arrive(phase, slot)
        if phase == 1 and s < PACKED:
            src, dst = ring.outs[1], ring.outs[2]
            p, q = lax.rem(slot, 2), lax.rem(slot, ring.depth(2))
            weights = {ring.axes[0]: 1, ring.axes[1]: 4}

            @pl.loop(0, 8)
            def _(n):
                blocks = [src[p, pl.ds(block_at(me, weights, {"z": n // 2, "x": lax.rem(n, 2) * 2 + half}), 128), :] for half in range(2)]
                rows = pick(n, blocks)
                at = pl.multiple_of(n * 80, 16)
                dst[q, pl.ds(at, 80), :] = rows[0:80]
                dst[q, pl.ds(at + 640, 80), :] = rows[80:160]
        else:
            ring.forward(phase, slot)
        ring.begin(phase + 1, slot)
        ring.close(phase, slot)

    def tables():
        experts = [(((me["z"] * 2 + c) * 4) + me["x"]).astype(f32) for c in (core, 1 - core)]

        @pl.loop(0, 8)
        def _(n):
            spots = [block_at(me, {"x": 1, "z": 4}, {"z": n // 2, "x": lax.rem(n, 2) * 2 + half}) // 4 for half in range(2)]
            blocks = [notes.outs[1][0, pl.ds(pl.multiple_of(at, 32), 32), :] for at in spots]

            def put_pick(source, hot):
                pick_ref[n, source * 80:source * 80 + 80, :] = hot

            def put_gain(source, gain):
                (gain_own, gain_send)[source][n] = gain
            pick_tables(blocks, experts, put_pick, put_gain)
        gains.start()

    def collect(s, slot):
        ring = rings[s]
        ring.arrive(2, slot)
        if s < PACKED:
            for part in range(4):
                pair(s, slot, part).start()
            return
        own, send = wares[s][:2]
        p = lax.rem(slot, ring.depth(2))
        weights = {axis: 4 ** i for i, axis in enumerate(ring.axes)}
        pl.when(slot >= 1)(lambda: pair(s, slot - 1).wait_send())

        @pl.loop(0, 8)
        def _(n):
            blocks = [jnp.concatenate([ring.outs[2][p, pl.ds(block_at(me, weights, {"z": n // 2, "x": lax.rem(n, 2) * 2 + half, "y": q}), 128), :]
                                       for q in range(4)], axis=1) for half in range(2)]
            rows = pick(n, blocks)
            at = pl.ds(pl.multiple_of(n * 80, 16), 80)
            own[at, :] = rows[0:80]
            send[at, :] = rows[80:160]
        pair(s, slot).start()
        pl.when(slot == ring.slots - 1)(lambda: pair(s, slot).wait_send())
        ring.close(2, slot)

    def multiply(s, slot):
        ring = rings[s]
        first = tile_of(s, slot)
        if s < PACKED:
            for part in range(4):
                pair(s, slot, part).wait_recv()
            got = wares[s][0]
            quarters = [lax.rem(me["y"] + part, 4) for part in range(4)]
            p = lax.rem(slot, ring.depth(2))
            rows = (jnp.concatenate([ring.outs[2][p, pl.ds(1280 * part, 640), :] for part in range(4)], axis=1),
                    jnp.concatenate([got[lax.rem(slot, 2), part] for part in range(4)], axis=1))
        else:
            pair(s, slot).wait_recv()
            quarters = range(4)
            rows = (wares[s][0][...], wares[s][2][lax.rem(slot, 2)])
        for w_ref, col in ((gate_ref, 0), (up_ref, 512)):
            w = jnp.concatenate([w_ref[pl.ds(pl.multiple_of(q * quarter + first, TILE), TILE), :] for q in quarters], axis=0)
            for half in range(2):
                total[half, :, col:col + 512] += jnp.dot(rows[half], w, preferred_element_type=f32)
        if s < PACKED:
            for part in range(4):
                pair(s, slot, part).wait_send()
            ring.close(2, slot)

    def stage(step, delay, body):
        for s, (_, _, slots) in enumerate(STREAMS):
            slot = step - delay
            pl.when((slot >= 0) & (slot < slots))(functools.partial(body, s, slot))

    def note(step, at, body):
        pl.when(step == at)(body)

    def note_open():
        notes.outs[0][0, 0:32, :] = meta_ref[...]
        notes.begin(0, 0)

    def note_pass():
        notes.arrive(0, 0)
        notes.forward(0, 0)
        notes.begin(1, 0)
        notes.close(0, 0)

    def note_end():
        notes.arrive(1, 0)
        tables()
        notes.close(1, 0)

    @pl.loop(0, max(slots for _, _, slots in STREAMS) + 6)
    def _(step):
        note(step, 4, note_end)
        note(step, 3, lambda: notes.middle(1, 0))
        note(step, 2, note_pass)
        note(step, 1, lambda: notes.middle(0, 0))
        note(step, 0, note_open)
        stage(step, 5, lambda s, slot: rings[s].middle(2, slot))
        stage(step, 4, lambda s, slot: pass_on(s, 1, slot))
        stage(step, 3, lambda s, slot: rings[s].middle(1, slot))
        stage(step, 2, lambda s, slot: pass_on(s, 0, slot))
        stage(step, 1, lambda s, slot: rings[s].middle(0, slot))
        stage(step, 0, open_tile)
        stage(step, 6, collect)

        @pl.when(step == 5)
        def _():
            total[...] = jnp.zeros_like(total)
            for load in loads:
                load.wait()

        stage(step, 6, multiply)

    gains.wait()

    @pl.loop(0, 8)
    def _(n):
        at = pl.ds(pl.multiple_of(n * 80, 16), 80)
        for half, ref, gain in ((0, own_ref, gain_own), (1, other_ref, gain_got)):
            gate = total[half, at, 0:512]
            upper = total[half, at, 512:1024]
            ref[at, :] = (jax.nn.silu(gate) * upper * gain[n][:, 0:1]).astype(bf16)


def rows_buffer(*shape):
    return pltpu.VMEM(shape + (TILE,), bf16)


def dispatch(tokens, meta, gate, up):
    vmem = pl.BlockSpec(memory_space=pltpu.VMEM)
    hbm = pl.BlockSpec(memory_space=pl.ANY)
    dma = pltpu.SemaphoreType.DMA
    hidden = jax.ShapeDtypeStruct((640, 512), bf16)
    scratch = [
        pltpu.VMEM(gate.shape, bf16), pltpu.VMEM(up.shape, bf16), pltpu.VMEM((2, 640, 1024), f32),
        pltpu.VMEM((8, 80, 128), f32), pltpu.VMEM((8, 80, 128), f32), pltpu.VMEM((8, 80, 128), f32),
        dma((2,)), dma((2,)), pltpu.SemaphoreType.REGULAR((len(STREAMS), 3, 2)),
    ]
    for s in range(len(STREAMS)):
        scratch += [rows_buffer(2, 512), rows_buffer(2, 2048), rows_buffer(3, 5120 if s < PACKED else 8192)]
        scratch += [dma((4, 2)), dma((4, 2)), dma((4, 3))] * 2
        if s < PACKED:
            scratch += [rows_buffer(2, 4, 640), dma((4,)), dma((2, 4))]
        else:
            scratch += [pltpu.VMEM((640, 512), bf16), pltpu.VMEM((640, 512), bf16), pltpu.VMEM((2, 640, 512), bf16), dma((1,)), dma((2,))]
    scratch += [rows_buffer(1, 128), rows_buffer(1, 512)] + [dma((4, 1))] * 4
    return pl.pallas_call(
        dispatch_kernel,
        out_shape=(hidden, hidden, jax.ShapeDtypeStruct((8, 160, 256), bf16)),
        in_specs=[vmem, vmem, hbm, hbm],
        out_specs=(vmem,) * 3,
        scratch_shapes=scratch,
        compiler_params=pltpu.CompilerParams(collective_id=0, has_side_effects=True, vmem_limit_bytes=66900000),
        name="dispatch",
    )(tokens, meta, gate, up)


class Reduce:
    def __init__(self, me, core, axes, ins, gots, mores, sends, recvs, credit, slots):
        self.me, self.core, self.axes = me, core, axes
        self.ins, self.gots, self.mores = ins, gots, mores
        self.sends, self.recvs, self.credit, self.slots = sends, recvs, credit, slots

    def copy(self, phase, slot, kind):
        p = lax.rem(slot, 2)
        buf = self.ins[phase].at[p]
        b = self.ins[phase].shape[1] // 4
        h = b // 2
        got, more = self.gots[phase], self.mores[phase]
        src, dst, step = (
            (pl.ds(b + h, b), got.at[p, 0], RIGHT),
            (pl.ds(2 * b + h, b), got.at[p, 1], LEFT),
            (pl.ds(b, h), more.at[p, 0], RIGHT),
            (pl.ds(3 * b + h, h), more.at[p, 1], LEFT),
        )[kind]
        return pltpu.make_async_remote_copy(
            src_ref=buf.at[src], dst_ref=dst, send_sem=self.sends.at[phase, kind, p], recv_sem=self.recvs.at[phase, kind, p],
            device_id=peer(self.me, self.core, self.axes[phase], step), device_id_type=MESH)

    def begin(self, phase, slot):
        pl.when(slot >= 2)(lambda: spend(self.credit, phase))
        self.copy(phase, slot, 0).start()
        self.copy(phase, slot, 1).start()

    def middle(self, phase, slot):
        p = lax.rem(slot, 2)
        buf, got = self.ins[phase], self.gots[phase]
        b = buf.shape[1] // 4
        h = b // 2
        for kind, base, skip in ((0, b, h), (1, 3 * b + h, 0)):
            self.copy(phase, slot, kind).wait_recv()

            def add(i, n):
                at = pl.ds(base + i, n)
                buf[p, at, :] = (buf[p, at, :].astype(f32) + got[p, kind, pl.ds(skip + i, n), :].astype(f32)).astype(bf16)
            tiles(h, add)
            self.copy(phase, slot, kind + 2).start()

    def finish(self, phase, slot, put):
        p = lax.rem(slot, 2)
        buf, got, more = self.ins[phase], self.gots[phase], self.mores[phase]
        b = buf.shape[1] // 4
        h = b // 2
        for kind, base, skip in ((0, 0, h), (1, h, 0)):
            self.copy(phase, slot, kind + 2).wait_recv()

            def add(i, n):
                at = base + i
                value = (buf[p, pl.ds(at, n), :].astype(f32) + got[p, 1 - kind, pl.ds(skip + i, n), :].astype(f32)
                         + more[p, kind, pl.ds(i, n), :].astype(f32))
                put(at, n, value.astype(bf16))
            tiles(h, add)

    def close(self, phase, slot):
        for kind in range(4):
            self.copy(phase, slot, kind).wait_send()
        pl.when(slot + 2 < self.slots)(lambda: grant(self.me, self.core, self.credit, phase, self.axes[phase]))


def combine_kernel(own_ref, other_ref, down_ref, pick_ref, out_ref, credit, *rest):
    rest = list(rest)

    def take(n):
        taken = rest[:n]
        del rest[:n]
        return taken

    me, core = place()
    partner = {"aa": me["z"] * 2 + (1 - core)}
    quarter = out_ref.shape[1]
    greet(me, core)
    rings, wares = [], []
    for s, (axes, _, slots) in enumerate(STREAMS):
        rings.append(Reduce(me, core, axes[::-1], take(3), take(3), take(3), *take(2), credit.at[s], slots))
        wares.append(take(6 if s < PACKED else 4))

    def pair(s, slot):
        p = lax.rem(slot, 2)
        if s < PACKED:
            _, src, got, _, send, recv = wares[s]
            dst = got.at[p]
        else:
            src, got, send, recv = wares[s]
            dst = got.at[p, :, pl.ds(80, 80)]
        return pltpu.make_async_remote_copy(
            src_ref=src, dst_ref=dst, send_sem=send.at[0], recv_sem=recv.at[p], device_id=partner, device_id_type=MESH)

    def tile_of(s, slot):
        return pl.multiple_of((slot + STREAMS[s][1]) * TILE, TILE)

    def project(s, slot):
        first = tile_of(s, slot)
        quarters = [lax.rem(me["y"] + part, 4) for part in range(4)] if s < PACKED else range(4)
        w = jnp.concatenate([down_ref[:, pl.ds(pl.multiple_of(q * quarter + first, TILE), TILE)] for q in quarters], axis=1)
        mine = jnp.dot(own_ref[...], w, preferred_element_type=f32).astype(bf16)
        if s < PACKED:
            for part in range(4):
                wares[s][0][part] = mine[:, part * TILE:(part + 1) * TILE]
        else:
            wares[s][1][lax.rem(slot, 2), :, 0:80, :] = mine.reshape(8, 80, 4 * TILE)
        pl.when(slot >= 1)(lambda: pair(s, slot - 1).wait_send())
        theirs = jnp.dot(other_ref[...], w, preferred_element_type=f32).astype(bf16)
        if s < PACKED:
            for part in range(4):
                wares[s][1][part] = theirs[:, part * TILE:(part + 1) * TILE]
        else:
            wares[s][0][...] = theirs.reshape(8, 80, 4 * TILE)
        pair(s, slot).start()
        pl.when(slot == rings[s].slots - 1)(lambda: pair(s, slot).wait_send())

    def spread(n, rows):
        return lax.dot_general(pick_ref[n], rows, (((0,), (0,)), ((), ())), preferred_element_type=f32).astype(bf16)

    def launch(s, slot):
        ring = rings[s]
        p = lax.rem(slot, 2)
        first_in = ring.ins[0]
        pair(s, slot).wait_recv()
        if s < PACKED:
            own, _, got = wares[s][:3]

            @pl.loop(0, 4)
            def _(part):
                at = pl.multiple_of(part * 1280, 1280)
                first_in[p, pl.ds(at, 640), :] = own[part]
                first_in[p, pl.ds(at + 640, 640), :] = got[p, part]
        else:
            weights = {axis: 4 ** (2 - i) for i, axis in enumerate(ring.axes)}

            @pl.loop(0, 8)
            def _(n):
                rows = spread(n, wares[s][1][p, n])
                for half in range(2):
                    for q in range(4):
                        at = block_at(me, weights, {"z": n // 2, "x": lax.rem(n, 2) * 2 + half, "y": q})
                        first_in[p, pl.ds(at, 128), :] = rows[half * 128:half * 128 + 128, q * TILE:(q + 1) * TILE]
        ring.begin(0, slot)

    def pass_on(s, phase, slot):
        ring = rings[s]
        dst, p = ring.ins[phase + 1], lax.rem(slot, 2)
        if phase == 0 and s < PACKED:
            summed = wares[s][3]

            def hold(at, n, value):
                summed[pl.ds(at, n), :] = value
            ring.finish(0, slot, hold)
            weights = {ring.axes[1]: 4, ring.axes[2]: 1}

            @pl.loop(0, 8)
            def _(n):
                at = pl.multiple_of(n * 80, 16)
                rows = spread(n, jnp.concatenate([summed[pl.ds(at, 80), :], summed[pl.ds(at + 640, 80), :]], axis=0))
                for half in range(2):
                    at = block_at(me, weights, {"z": n // 2, "x": lax.rem(n, 2) * 2 + half})
                    dst[p, pl.ds(at, 128), :] = rows[half * 128:half * 128 + 128]
        else:
            def put(at, n, value):
                dst[p, pl.ds(at, n), :] = value
            ring.finish(phase, slot, put)
        ring.begin(phase + 1, slot)
        ring.close(phase, slot)

    def deliver(s, slot):
        def put(at, n, value):
            out_ref[pl.ds(at, n), pl.ds(tile_of(s, slot), TILE)] = value
        rings[s].finish(2, slot, put)
        rings[s].close(2, slot)

    def stage(step, delay, body, lowest=0):
        for s, (_, _, slots) in enumerate(STREAMS):
            slot = step - delay
            pl.when((slot >= lowest) & (slot < slots))(functools.partial(body, s, slot))

    order = (2, 0, 3, 1)
    start = jnp.int32(0)
    project(order[0], start)
    for before, s in zip(order, order[1:]):
        project(s, start)
        launch(before, start)
    launch(order[-1], start)

    @pl.loop(0, max(slots for _, _, slots in STREAMS) + 6)
    def _(step):
        stage(step, 1, lambda s, slot: rings[s].middle(0, slot))
        stage(step, 3, lambda s, slot: rings[s].middle(1, slot))
        stage(step, 5, lambda s, slot: rings[s].middle(2, slot))
        stage(step, 6, deliver)
        stage(step, 4, lambda s, slot: pass_on(s, 1, slot))
        stage(step, 2, lambda s, slot: pass_on(s, 0, slot))
        stage(step, 0, launch, 1)
        stage(step, -1, project, 1)


def combine(own, other, down, pick):
    quarter = down.shape[1] // 4
    vmem = pl.BlockSpec(memory_space=pltpu.VMEM)
    dma = pltpu.SemaphoreType.DMA
    scratch = [pltpu.SemaphoreType.REGULAR((len(STREAMS), 3, 2))]
    for s in range(len(STREAMS)):
        sizes = (5120 if s < PACKED else 8192, 2048, 512)
        scratch += [rows_buffer(2, n) for n in sizes]
        scratch += [rows_buffer(2, 2, n // 4) for n in sizes]
        scratch += [rows_buffer(2, 2, n // 8) for n in sizes]
        scratch += [dma((3, 4, 2))] * 2
        if s < PACKED:
            scratch += [rows_buffer(4, 640), rows_buffer(4, 640), rows_buffer(2, 4, 640), rows_buffer(1280), dma((1,)), dma((2,))]
        else:
            scratch += [pltpu.VMEM((8, 80, 512), bf16), pltpu.VMEM((2, 8, 160, 512), bf16), dma((1,)), dma((2,))]
    return pl.pallas_call(
        combine_kernel,
        out_shape=jax.ShapeDtypeStruct((128, quarter), bf16),
        in_specs=[vmem] * 4,
        out_specs=vmem,
        scratch_shapes=scratch,
        compiler_params=pltpu.CompilerParams(collective_id=1, has_side_effects=True, vmem_limit_bytes=66900000),
        name="combine",
    )(own, other, down, pick)


def on_device(tokens, routing, gate_codes, w_gate, w_up, w_down):
    codes = jnp.concatenate([routing, gate_codes // 256, gate_codes % 256], axis=1).astype(bf16).T
    meta = jnp.pad(codes, ((0, 32 - codes.shape[0]), (0, 0)))
    own, other, pick = dispatch(tokens, meta, w_gate[0], w_up[0])
    return combine(own, other, w_down[0], pick)


def solution(mesh):
    return jax.shard_map(
        on_device,
        mesh=mesh,
        in_specs=(
            P(("aa", "col"), "ba"),
            P(("aa", "col"), None),
            P(("aa", "col"), None),
            P(("aa", "col"), None, "ba"),
            P(("aa", "col"), None, "ba"),
            P(("aa", "col"), "ba", None),
        ),
        out_specs=P(("aa", "col"), "ba"),
        check_vma=False,
    )
```

```python
import functools
import jax
import jax.numpy as jnp
from jax import lax
from jax.experimental import pallas as pl
from jax.experimental.pallas import tpu as pltpu
from jax.sharding import PartitionSpec as P

MESH = pl.DeviceIdType.MESH
route_scale = 2.827
bf16 = jnp.bfloat16
f32 = jnp.float32
TILE = 128
STREAMS = ((("z", "x", "y"), 0, 4), (("x", "z", "y"), 4, 4), (("y", "z", "x"), 8, 3), (("y", "x", "z"), 11, 3))
PACKED = 2
RIGHT, LEFT, ACROSS = 1, -1, 2


def place():
    aa = lax.axis_index("aa")
    return {"z": aa // 2, "y": lax.axis_index("ba"), "x": lax.axis_index("col")}, aa % 2


def peer(me, core, axis, step):
    at = lax.rem(me[axis] + (step + 4), 4)
    if axis == "z":
        return {"aa": at * 2 + core}
    return {"ba": at} if axis == "y" else {"col": at}


def greet(me, core):
    barrier = pltpu.get_barrier_semaphore()
    for axis in "xyz":
        for step in (RIGHT, LEFT, ACROSS):
            pl.semaphore_signal(barrier, inc=1, device_id=peer(me, core, axis, step), device_id_type=MESH)
    pl.semaphore_signal(barrier, inc=1, device_id={"aa": me["z"] * 2 + (1 - core)}, device_id_type=MESH)
    pl.semaphore_wait(barrier, 10)


def grant(me, core, credit, phase, axis, direct):
    for i, step in enumerate((RIGHT, LEFT, ACROSS)[:3 if direct else 2]):
        pl.semaphore_signal(credit.at[phase, i], inc=1, device_id=peer(me, core, axis, step), device_id_type=MESH)


def spend(credit, phase, direct):
    for i in range(3 if direct else 2):
        pl.semaphore_wait(credit.at[phase, i], 1)


def tiles(rows, body):
    size = min(rows, 128 if rows % 256 else 256)
    if rows == size:
        body(0, size)
    else:
        @pl.loop(0, rows // size)
        def _(i):
            body(pl.multiple_of(i * size, size), size)


def block_at(me, weights, there):
    at = sum(lax.rem(spot - me[axis] + 4, 4) * weights[axis] for axis, spot in there.items())
    return pl.multiple_of(at * 128, 128)


def pick_tables(blocks, experts, put_pick, put_gain):
    lane = lax.broadcasted_iota(jnp.int32, (128, 128), 1)
    row = lax.broadcasted_iota(jnp.int32, (128, 128), 0)
    before = (row < lane).astype(bf16)
    slot_row = lax.broadcasted_iota(jnp.int32, (80, 256), 0)
    half_lane = lax.broadcasted_iota(jnp.int32, (80, 256), 1)
    second_row, second_lane = slot_row >= 40, half_lane >= 128
    position = jnp.where(second_row, slot_row - 40, slot_row).astype(f32)
    same = second_row == second_lane
    for source, expert in enumerate(experts):
        taken, pos, gain = [], [], []
        for block in blocks:
            block = block.astype(f32)
            code = block[8:16] * 256.0 + block[16:24]
            weight = route_scale * code / jnp.sum(code, axis=0, keepdims=True)
            named = block[0:8] == expert
            hit = jnp.max(jnp.where(named, 1.0, 0.0), axis=0, keepdims=True)
            taken.append(hit)
            wide = jnp.broadcast_to(hit, (8, 128)).astype(bf16)
            pos.append(jnp.dot(wide, before, preferred_element_type=f32)[0:1])
            gain.append(jnp.sum(jnp.where(named, weight, 0.0), axis=0, keepdims=True))
        taken, pos, gain = (jnp.concatenate(v, axis=1) for v in (taken, pos, gain))
        hot = same & (pos == position) & (taken > 0.5)
        put_pick(source, jnp.where(hot, 1.0, 0.0).astype(bf16))
        put_gain(source, jnp.broadcast_to(jnp.sum(jnp.where(hot, gain, 0.0), axis=1, keepdims=True), (80, 128)))


class Gather:
    def __init__(self, me, core, axes, direct, outs, sends, recvs, credit, slots):
        self.me, self.core, self.axes, self.direct, self.outs = me, core, axes, direct, outs
        self.sends, self.recvs, self.credit, self.slots = sends, recvs, credit, slots

    def depth(self, phase):
        return self.outs[phase].shape[0]

    def copy(self, phase, slot, kind):
        p = lax.rem(slot, self.depth(phase))
        buf = self.outs[phase].at[p]
        b = self.outs[phase].shape[1] // 4
        h = b // 2
        src, dst, step = (
            (pl.ds(0, b), pl.ds(3 * b, b), RIGHT),
            (pl.ds(0, b), pl.ds(b, b), LEFT),
            (pl.ds(3 * b, h), pl.ds(2 * b, h), RIGHT),
            (pl.ds(b + h, h), pl.ds(2 * b + h, h), LEFT),
            (pl.ds(0, b), pl.ds(2 * b, b), ACROSS),
        )[4 if self.direct[phase] and kind == 2 else kind]
        return pltpu.make_async_remote_copy(
            src_ref=buf.at[src], dst_ref=buf.at[dst], send_sem=self.sends[phase].at[kind, p], recv_sem=self.recvs[phase].at[kind, p],
            device_id=peer(self.me, self.core, self.axes[phase], step), device_id_type=MESH)

    def begin(self, phase, slot):
        if self.slots > self.depth(phase):
            pl.when(slot >= self.depth(phase))(lambda: spend(self.credit, phase, self.direct[phase]))
        for kind in range(3 if self.direct[phase] else 2):
            self.copy(phase, slot, kind).start()

    def middle(self, phase, slot):
        self.copy(phase, slot, 0).wait_recv()
        self.copy(phase, slot, 2).start()
        self.copy(phase, slot, 1).wait_recv()
        self.copy(phase, slot, 3).start()

    def arrive(self, phase, slot):
        for kind in (0, 1, 2) if self.direct[phase] else (2, 3):
            self.copy(phase, slot, kind).wait_recv()

    def close(self, phase, slot):
        for kind in range(3 if self.direct[phase] else 4):
            self.copy(phase, slot, kind).wait_send()
        if self.slots > self.depth(phase):
            pl.when(slot + self.depth(phase) < self.slots)(
                lambda: grant(self.me, self.core, self.credit, phase, self.axes[phase], self.direct[phase]))

    def forward(self, phase, slot):
        src, dst = self.outs[phase], self.outs[phase + 1]
        p, q = lax.rem(slot, src.shape[0]), lax.rem(slot, dst.shape[0])

        def move(at, n):
            dst[q, pl.ds(at, n), :] = src[p, pl.ds(at, n), :]
        tiles(src.shape[1], move)


def dispatch_kernel(tok_ref, routing_ref, codes_ref, gate_hbm, up_hbm, own_ref, other_ref, pick_ref,
                    gate_ref, up_ref, total, gain_own, gain_send, gain_got, gain_sem, load_sem, credit, *rest):
    rest = list(rest)

    def take(n):
        taken = rest[:n]
        del rest[:n]
        return taken

    me, core = place()
    partner = {"aa": me["z"] * 2 + (1 - core)}
    quarter = tok_ref.shape[1]
    loads = [pltpu.make_async_copy(gate_hbm, gate_ref, load_sem.at[0]), pltpu.make_async_copy(up_hbm, up_ref, load_sem.at[1])]
    for load in loads:
        load.start()
    greet(me, core)
    rings, wares = [], []
    for s, (axes, _, slots) in enumerate(STREAMS):
        rings.append(Gather(me, core, axes, (True, False, False), take(3), take(3), take(3), credit.at[s], slots))
        wares.append(take(3 if s < PACKED else 5))
    notes = Gather(me, core, ("x", "z"), (True, True), take(2), take(2), take(2), None, 1)
    gains = pltpu.make_async_remote_copy(
        src_ref=gain_send, dst_ref=gain_got, send_sem=gain_sem.at[0], recv_sem=gain_sem.at[1],
        device_id=partner, device_id_type=MESH)

    def pair(s, slot, part=0):
        if s < PACKED:
            got, send, recv = wares[s]
            b = got.shape[2]
            src = rings[s].outs[2].at[lax.rem(slot, rings[s].depth(2)), pl.ds(2 * b * part + b, b)]
            dst = got.at[lax.rem(slot, 2), part]
            send_at, recv_at = send.at[part], recv.at[lax.rem(slot, 2), part]
        else:
            _, src, got, send, recv = wares[s]
            dst = got.at[lax.rem(slot, 2)]
            send_at, recv_at = send.at[0], recv.at[lax.rem(slot, 2)]
        return pltpu.make_async_remote_copy(
            src_ref=src, dst_ref=dst, send_sem=send_at, recv_sem=recv_at, device_id=partner, device_id_type=MESH)

    def tile_of(s, slot):
        return pl.multiple_of((slot + STREAMS[s][1]) * TILE, TILE)

    def open_tile(s, slot):
        rings[s].outs[0][lax.rem(slot, 2), 0:128, :] = tok_ref[:, pl.ds(tile_of(s, slot), TILE)]
        rings[s].begin(0, slot)

    def pick(n, blocks):
        return jnp.dot(pick_ref[n], jnp.concatenate(blocks, axis=0), preferred_element_type=f32).astype(bf16)

    def pass_on(s, phase, slot):
        ring = rings[s]
        ring.arrive(phase, slot)
        if phase == 1 and s < PACKED:
            src, dst = ring.outs[1], ring.outs[2]
            p, q = lax.rem(slot, ring.depth(1)), lax.rem(slot, ring.depth(2))
            weights = {ring.axes[0]: 1, ring.axes[1]: 4}

            @pl.loop(0, 8)
            def _(n):
                blocks = [src[p, pl.ds(block_at(me, weights, {"z": n // 2, "x": lax.rem(n, 2) * 2 + half}), 128), :] for half in range(2)]
                rows = pick(n, blocks)
                at = pl.multiple_of(n * 80, 16)
                dst[q, pl.ds(at, 80), :] = rows[0:80]
                dst[q, pl.ds(at + 640, 80), :] = rows[80:160]
        else:
            ring.forward(phase, slot)
        ring.begin(phase + 1, slot)
        ring.close(phase, slot)

    def tables():
        experts = [(((me["z"] * 2 + c) * 4) + me["x"]).astype(f32) for c in (core, 1 - core)]

        @pl.loop(0, 8)
        def _(n):
            spots = [block_at(me, {"x": 1, "z": 4}, {"z": n // 2, "x": lax.rem(n, 2) * 2 + half}) // 4 for half in range(2)]
            blocks = [notes.outs[1][0, pl.ds(pl.multiple_of(at, 32), 32), :] for at in spots]

            def put_pick(source, hot):
                pick_ref[n, source * 80:source * 80 + 80, :] = hot

            def put_gain(source, gain):
                (gain_own, gain_send)[source][n] = gain
            pick_tables(blocks, experts, put_pick, put_gain)
        gains.start()

    def collect(s, slot):
        ring = rings[s]
        ring.arrive(2, slot)
        if s < PACKED:
            for part in range(4):
                pair(s, slot, part).start()
            return
        own, send = wares[s][:2]
        p = lax.rem(slot, ring.depth(2))
        weights = {axis: 4 ** i for i, axis in enumerate(ring.axes)}
        pl.when(slot >= 1)(lambda: pair(s, slot - 1).wait_send())

        @pl.loop(0, 8)
        def _(n):
            blocks = [jnp.concatenate([ring.outs[2][p, pl.ds(block_at(me, weights, {"z": n // 2, "x": lax.rem(n, 2) * 2 + half, "y": q}), 128), :]
                                       for q in range(4)], axis=1) for half in range(2)]
            rows = pick(n, blocks)
            at = pl.ds(pl.multiple_of(n * 80, 16), 80)
            own[at, :] = rows[0:80]
            send[at, :] = rows[80:160]
        pair(s, slot).start()
        pl.when(slot == ring.slots - 1)(lambda: pair(s, slot).wait_send())
        ring.close(2, slot)

    def multiply(s, slot):
        ring = rings[s]
        first = tile_of(s, slot)
        if s < PACKED:
            for part in range(4):
                pair(s, slot, part).wait_recv()
            got = wares[s][0]
            quarters = [lax.rem(me["y"] + part, 4) for part in range(4)]
            p = lax.rem(slot, ring.depth(2))
            rows = (jnp.concatenate([ring.outs[2][p, pl.ds(1280 * part, 640), :] for part in range(4)], axis=1),
                    jnp.concatenate([got[lax.rem(slot, 2), part] for part in range(4)], axis=1))
        else:
            pair(s, slot).wait_recv()
            quarters = range(4)
            rows = (wares[s][0][...], wares[s][2][lax.rem(slot, 2)])
        for w_ref, col in ((gate_ref, 0), (up_ref, 512)):
            w = jnp.concatenate([w_ref[pl.ds(pl.multiple_of(q * quarter + first, TILE), TILE), :] for q in quarters], axis=0)
            for half in range(2):
                total[half, :, col:col + 512] += jnp.dot(rows[half], w, preferred_element_type=f32)
        if s < PACKED:
            for part in range(4):
                pair(s, slot, part).wait_send()
            ring.close(2, slot)

    def stage(step, delay, body):
        for s, (_, _, slots) in enumerate(STREAMS):
            slot = step - delay
            pl.when((slot >= 0) & (slot < slots))(functools.partial(body, s, slot))

    def note(step, at, body):
        pl.when(step == at)(body)

    def note_open():
        nothing = jnp.zeros((128, 112), f32)
        both = jnp.concatenate([routing_ref[...].astype(f32), codes_ref[...].astype(f32), nothing], axis=1).T
        high = jnp.floor(both[8:16] * (1.0 / 256.0))
        notes.outs[0][0, 0:32, :] = jnp.concatenate(
            [both[0:8], high, both[8:16] - 256.0 * high, both[16:24]], axis=0).astype(bf16)
        notes.begin(0, 0)

    def note_pass():
        notes.arrive(0, 0)
        notes.forward(0, 0)
        notes.begin(1, 0)
        notes.close(0, 0)

    def note_end():
        notes.arrive(1, 0)
        tables()
        notes.close(1, 0)

    def consume(step):
        def one(s, body):
            slot = step - 5
            pl.when((slot >= 0) & (slot < STREAMS[s][2]))(lambda: body(s, slot))

        for s in (2, 3, 0):
            one(s, collect)
        for s in (2, 3, 0):
            one(s, multiply)
        one(1, collect)
        one(1, multiply)

    @pl.loop(0, max(slots for _, _, slots in STREAMS) + 5)
    def _(step):
        note(step, 2, note_end)
        note(step, 1, note_pass)
        note(step, 0, note_open)
        stage(step, 2, lambda s, slot: rings[s].middle(1, slot))
        stage(step, 1, lambda s, slot: pass_on(s, 0, slot))
        stage(step, 0, open_tile)
        stage(step, 4, lambda s, slot: rings[s].middle(2, slot))
        stage(step, 3, lambda s, slot: pass_on(s, 1, slot))

        @pl.when(step == 4)
        def _():
            total[...] = jnp.zeros_like(total)
            for load in loads:
                load.wait()

        consume(step)

    gains.wait()

    @pl.loop(0, 8)
    def _(n):
        at = pl.ds(pl.multiple_of(n * 80, 16), 80)
        for half, ref, gain in ((0, own_ref, gain_own), (1, other_ref, gain_got)):
            gate = total[half, at, 0:512]
            upper = total[half, at, 512:1024]
            ref[at, :] = (jax.nn.silu(gate) * upper * gain[n][:, 0:1]).astype(bf16)


def rows_buffer(*shape):
    return pltpu.VMEM(shape + (TILE,), bf16)


def dispatch(tokens, routing, codes, gate, up):
    vmem = pl.BlockSpec(memory_space=pltpu.VMEM)
    hbm = pl.BlockSpec(memory_space=pl.ANY)
    dma = pltpu.SemaphoreType.DMA
    hidden = jax.ShapeDtypeStruct((640, 512), bf16)
    scratch = [
        pltpu.VMEM(gate.shape, bf16), pltpu.VMEM(up.shape, bf16), pltpu.VMEM((2, 640, 1024), f32),
        pltpu.VMEM((8, 80, 128), f32), pltpu.VMEM((8, 80, 128), f32), pltpu.VMEM((8, 80, 128), f32),
        dma((2,)), dma((2,)), pltpu.SemaphoreType.REGULAR((len(STREAMS), 3, 3)),
    ]
    for s in range(len(STREAMS)):
        scratch += [rows_buffer(2, 512), rows_buffer(3, 2048), rows_buffer(3, 5120 if s < PACKED else 8192)]
        scratch += [dma((4, 2)), dma((4, 3)), dma((4, 3))] * 2
        if s < PACKED:
            scratch += [rows_buffer(2, 4, 640), dma((4,)), dma((2, 4))]
        else:
            scratch += [pltpu.VMEM((640, 512), bf16), pltpu.VMEM((640, 512), bf16), pltpu.VMEM((2, 640, 512), bf16), dma((1,)), dma((2,))]
    scratch += [rows_buffer(1, 128), rows_buffer(1, 512)] + [dma((4, 1))] * 4
    return pl.pallas_call(
        dispatch_kernel,
        out_shape=(hidden, hidden, jax.ShapeDtypeStruct((8, 160, 256), bf16)),
        in_specs=[vmem, vmem, vmem, hbm, hbm],
        out_specs=(vmem,) * 3,
        scratch_shapes=scratch,
        compiler_params=pltpu.CompilerParams(collective_id=0, has_side_effects=True, vmem_limit_bytes=66900000),
        name="dispatch",
    )(tokens, routing, codes, gate, up)


class Reduce:
    def __init__(self, me, core, axes, direct, ins, gots, mores, sends, recvs, credit, slots):
        self.me, self.core, self.axes, self.direct = me, core, axes, direct
        self.ins, self.gots, self.mores = ins, gots, mores
        self.sends, self.recvs, self.credit, self.slots = sends, recvs, credit, slots

    def depth(self, phase):
        return self.ins[phase].shape[0]

    def copy(self, phase, slot, kind):
        p = lax.rem(slot, self.depth(phase))
        buf = self.ins[phase].at[p]
        b = self.ins[phase].shape[1] // 4
        h = b // 2
        got, more = self.gots[phase], self.mores[phase]
        if self.direct[phase]:
            src, dst, step = (
                (pl.ds(b, b), got.at[p, 0], RIGHT),
                (pl.ds(3 * b, b), got.at[p, 1], LEFT),
                (pl.ds(2 * b, b), more.at[p, 0], ACROSS),
            )[kind]
        else:
            src, dst, step = (
                (pl.ds(b + h, b), got.at[p, 0], RIGHT),
                (pl.ds(2 * b + h, b), got.at[p, 1], LEFT),
                (pl.ds(b, h), more.at[p, 0], RIGHT),
                (pl.ds(3 * b + h, h), more.at[p, 1], LEFT),
            )[kind]
        return pltpu.make_async_remote_copy(
            src_ref=buf.at[src], dst_ref=dst, send_sem=self.sends[phase].at[kind, p], recv_sem=self.recvs[phase].at[kind, p],
            device_id=peer(self.me, self.core, self.axes[phase], step), device_id_type=MESH)

    def begin(self, phase, slot):
        if self.slots > self.depth(phase):
            pl.when(slot >= self.depth(phase))(lambda: spend(self.credit, phase, self.direct[phase]))
        for kind in range(3 if self.direct[phase] else 2):
            self.copy(phase, slot, kind).start()

    def middle(self, phase, slot):
        p = lax.rem(slot, self.depth(phase))
        buf, got = self.ins[phase], self.gots[phase]
        b = buf.shape[1] // 4
        h = b // 2
        for kind, base, skip in ((0, b, h), (1, 3 * b + h, 0)):
            self.copy(phase, slot, kind).wait_recv()

            def add(i, n):
                at = pl.ds(base + i, n)
                buf[p, at, :] = (buf[p, at, :].astype(f32) + got[p, kind, pl.ds(skip + i, n), :].astype(f32)).astype(bf16)
            tiles(h, add)
            self.copy(phase, slot, kind + 2).start()

    def finish(self, phase, slot, put):
        p = lax.rem(slot, self.depth(phase))
        buf, got, more = self.ins[phase], self.gots[phase], self.mores[phase]
        b = buf.shape[1] // 4
        h = b // 2
        if self.direct[phase]:
            for kind in range(3):
                self.copy(phase, slot, kind).wait_recv()

            def add_all(at, n):
                value = ((buf[p, pl.ds(at, n), :].astype(f32) + got[p, 0, pl.ds(at, n), :].astype(f32))
                         + (got[p, 1, pl.ds(at, n), :].astype(f32) + more[p, 0, pl.ds(at, n), :].astype(f32)))
                put(at, n, value.astype(bf16))
            tiles(b, add_all)
            return
        for kind, base, skip in ((0, 0, h), (1, h, 0)):
            self.copy(phase, slot, kind + 2).wait_recv()

            def add(i, n):
                at = base + i
                value = (buf[p, pl.ds(at, n), :].astype(f32) + got[p, 1 - kind, pl.ds(skip + i, n), :].astype(f32)
                         + more[p, kind, pl.ds(i, n), :].astype(f32))
                put(at, n, value.astype(bf16))
            tiles(h, add)

    def close(self, phase, slot):
        for kind in range(3 if self.direct[phase] else 4):
            self.copy(phase, slot, kind).wait_send()
        if self.slots > self.depth(phase):
            pl.when(slot + self.depth(phase) < self.slots)(
                lambda: grant(self.me, self.core, self.credit, phase, self.axes[phase], self.direct[phase]))


def combine_kernel(own_ref, other_ref, down_hbm, pick_ref, out_ref, down_ref, load_sem, credit, *rest):
    rest = list(rest)

    def take(n):
        taken = rest[:n]
        del rest[:n]
        return taken

    me, core = place()
    partner = {"aa": me["z"] * 2 + (1 - core)}
    quarter = out_ref.shape[1]
    order = (0, 2, 1, 3)

    def load(s, slot, part):
        q = lax.rem(me["y"] + part, 4) if s < PACKED else part
        at = slot + STREAMS[s][1]
        return pltpu.make_async_copy(
            down_hbm.at[:, pl.ds(pl.multiple_of(q * quarter + at * TILE, TILE), TILE)],
            down_ref.at[at, :, pl.ds(part * TILE, TILE)], load_sem.at[at, part])

    for slot in range(max(slots for _, _, slots in STREAMS)):
        for s in order:
            if slot < STREAMS[s][2]:
                for part in range(4):
                    load(s, slot, part).start()
    greet(me, core)
    rings, wares = [], []
    for s, (axes, _, slots) in enumerate(STREAMS):
        rings.append(Reduce(me, core, axes[::-1], (False, False, True), take(3), take(3), take(3), take(3), take(3), credit.at[s], slots))
        wares.append(take(6 if s < PACKED else 4))

    def pair(s, slot):
        p = lax.rem(slot, 2)
        if s < PACKED:
            _, src, got, _, send, recv = wares[s]
            dst = got.at[p]
        else:
            src, got, send, recv = wares[s]
            dst = got.at[p, :, pl.ds(80, 80)]
        return pltpu.make_async_remote_copy(
            src_ref=src, dst_ref=dst, send_sem=send.at[0], recv_sem=recv.at[p], device_id=partner, device_id_type=MESH)

    def tile_of(s, slot):
        return pl.multiple_of((slot + STREAMS[s][1]) * TILE, TILE)

    def project(s, slot):
        for part in range(4):
            load(s, slot, part).wait()
        w = down_ref[slot + STREAMS[s][1]]
        mine = jnp.dot(own_ref[...], w, preferred_element_type=f32).astype(bf16)
        if s < PACKED:
            for part in range(4):
                wares[s][0][part] = mine[:, part * TILE:(part + 1) * TILE]
        else:
            wares[s][1][lax.rem(slot, 2), :, 0:80, :] = mine.reshape(8, 80, 4 * TILE)
        pl.when(slot >= 1)(lambda: pair(s, slot - 1).wait_send())
        theirs = jnp.dot(other_ref[...], w, preferred_element_type=f32).astype(bf16)
        if s < PACKED:
            for part in range(4):
                wares[s][1][part] = theirs[:, part * TILE:(part + 1) * TILE]
        else:
            wares[s][0][...] = theirs.reshape(8, 80, 4 * TILE)
        pair(s, slot).start()
        pl.when(slot == rings[s].slots - 1)(lambda: pair(s, slot).wait_send())

    def spread(n, rows):
        return lax.dot_general(pick_ref[n], rows, (((0,), (0,)), ((), ())), preferred_element_type=f32).astype(bf16)

    def launch(s, slot):
        ring = rings[s]
        p, d = lax.rem(slot, ring.depth(0)), lax.rem(slot, 2)
        first_in = ring.ins[0]
        pair(s, slot).wait_recv()
        if s < PACKED:
            own, _, got = wares[s][:3]

            @pl.loop(0, 4)
            def _(part):
                at = pl.multiple_of(part * 1280, 1280)
                first_in[p, pl.ds(at, 640), :] = own[part]
                first_in[p, pl.ds(at + 640, 640), :] = got[d, part]
        else:
            weights = {axis: 4 ** (2 - i) for i, axis in enumerate(ring.axes)}

            @pl.loop(0, 8)
            def _(n):
                rows = spread(n, wares[s][1][d, n])
                for half in range(2):
                    for q in range(4):
                        at = block_at(me, weights, {"z": n // 2, "x": lax.rem(n, 2) * 2 + half, "y": q})
                        first_in[p, pl.ds(at, 128), :] = rows[half * 128:half * 128 + 128, q * TILE:(q + 1) * TILE]
        ring.begin(0, slot)

    def pass_on(s, phase, slot):
        ring = rings[s]
        dst, p = ring.ins[phase + 1], lax.rem(slot, 2)
        if phase == 0 and s < PACKED:
            summed = wares[s][3]

            def hold(at, n, value):
                summed[pl.ds(at, n), :] = value
            ring.finish(0, slot, hold)
            weights = {ring.axes[1]: 4, ring.axes[2]: 1}

            @pl.loop(0, 8)
            def _(n):
                at = pl.multiple_of(n * 80, 16)
                rows = spread(n, jnp.concatenate([summed[pl.ds(at, 80), :], summed[pl.ds(at + 640, 80), :]], axis=0))
                for half in range(2):
                    at = block_at(me, weights, {"z": n // 2, "x": lax.rem(n, 2) * 2 + half})
                    dst[p, pl.ds(at, 128), :] = rows[half * 128:half * 128 + 128]
        else:
            def put(at, n, value):
                dst[p, pl.ds(at, n), :] = value
            ring.finish(phase, slot, put)
        ring.begin(phase + 1, slot)
        ring.close(phase, slot)

    def deliver(s, slot):
        def put(at, n, value):
            out_ref[pl.ds(at, n), pl.ds(tile_of(s, slot), TILE)] = value
        rings[s].finish(2, slot, put)
        rings[s].close(2, slot)

    def stage(step, delay, body, lowest=0, streams=range(len(STREAMS))):
        for s in streams:
            slot = step - delay
            pl.when((slot >= lowest) & (slot < STREAMS[s][2]))(functools.partial(body, s, slot))

    start = jnp.int32(0)
    project(order[0], start)
    for before, s in zip(order, order[1:]):
        project(s, start)
        launch(before, start)
    launch(order[-1], start)
    packed, plain = range(PACKED), range(PACKED, len(STREAMS))

    @pl.loop(0, max(slots for _, _, slots in STREAMS) + 5)
    def _(step):
        stage(step, 1, lambda s, slot: rings[s].middle(0, slot))
        stage(step, 0, launch, 1, packed)
        stage(step, 3, lambda s, slot: rings[s].middle(1, slot))
        stage(step, 5, deliver)
        stage(step, 4, lambda s, slot: pass_on(s, 1, slot))
        for s in plain:
            stage(step, 2, lambda s, slot: pass_on(s, 0, slot), 0, (s,))
            stage(step, 0, launch, 1, (s,))
        stage(step, 2, lambda s, slot: pass_on(s, 0, slot), 0, packed)
        stage(step, -1, project, 1)


def combine(own, other, down, pick):
    quarter = down.shape[1] // 4
    vmem = pl.BlockSpec(memory_space=pltpu.VMEM)
    dma = pltpu.SemaphoreType.DMA
    count = quarter // TILE
    scratch = [pltpu.VMEM((count, down.shape[0], 4 * TILE), bf16), dma((count, 4)), pltpu.SemaphoreType.REGULAR((len(STREAMS), 3, 3))]
    for s in range(len(STREAMS)):
        sizes = (5120 if s < PACKED else 8192, 2048, 512)
        depths = (3 if s < PACKED else 2, 2, 2)
        scratch += [rows_buffer(d, n) for d, n in zip(depths, sizes)]
        scratch += [rows_buffer(d, 2, n // 4) for d, n in zip(depths, sizes)]
        scratch += [rows_buffer(depths[0], 2, sizes[0] // 8), rows_buffer(2, 2, sizes[1] // 8), rows_buffer(2, 1, sizes[2] // 4)]
        scratch += [dma((4, d)) for d in depths] * 2
        if s < PACKED:
            scratch += [rows_buffer(4, 640), rows_buffer(4, 640), rows_buffer(2, 4, 640), rows_buffer(1280), dma((1,)), dma((2,))]
        else:
            scratch += [pltpu.VMEM((8, 80, 512), bf16), pltpu.VMEM((2, 8, 160, 512), bf16), dma((1,)), dma((2,))]
    return pl.pallas_call(
        combine_kernel,
        out_shape=jax.ShapeDtypeStruct((128, quarter), bf16),
        in_specs=[vmem, vmem, pl.BlockSpec(memory_space=pl.ANY), vmem],
        out_specs=vmem,
        scratch_shapes=scratch,
        compiler_params=pltpu.CompilerParams(collective_id=1, has_side_effects=True, vmem_limit_bytes=66900000),
        name="combine",
    )(own, other, down, pick)


def on_device(tokens, routing, gate_codes, w_gate, w_up, w_down):
    own, other, pick = dispatch(tokens, routing, gate_codes, w_gate[0], w_up[0])
    return combine(own, other, w_down[0], pick)


def solution(mesh):
    return jax.shard_map(
        on_device,
        mesh=mesh,
        in_specs=(
            P(("aa", "col"), "ba"),
            P(("aa", "col"), None),
            P(("aa", "col"), None),
            P(("aa", "col"), None, "ba"),
            P(("aa", "col"), None, "ba"),
            P(("aa", "col"), "ba", None),
        ),
        out_specs=P(("aa", "col"), "ba"),
        check_vma=False,
    )
```

```python
import functools
import jax
import jax.numpy as jnp
from jax import lax
from jax.experimental import pallas as pl
from jax.experimental.pallas import tpu as pltpu
from jax.sharding import PartitionSpec as P

MESH = pl.DeviceIdType.MESH
route_scale = 2.827
bf16 = jnp.bfloat16
f32 = jnp.float32
TILE = 128
STREAMS = ((("z", "x", "y"), 0, 4), (("x", "z", "y"), 4, 4), (("y", "z", "x"), 8, 3), (("y", "x", "z"), 11, 3))
PACKED = 2
RIGHT, LEFT, ACROSS = 1, -1, 2


def place():
    aa = lax.axis_index("aa")
    return {"z": aa // 2, "y": lax.axis_index("ba"), "x": lax.axis_index("col")}, aa % 2


def peer(me, core, axis, step):
    at = lax.rem(me[axis] + (step + 4), 4)
    if axis == "z":
        return {"aa": at * 2 + core}
    return {"ba": at} if axis == "y" else {"col": at}


def greet(me, core):
    barrier = pltpu.get_barrier_semaphore()
    for axis in "xyz":
        for step in (RIGHT, LEFT, ACROSS):
            pl.semaphore_signal(barrier, inc=1, device_id=peer(me, core, axis, step), device_id_type=MESH)
    pl.semaphore_signal(barrier, inc=1, device_id={"aa": me["z"] * 2 + (1 - core)}, device_id_type=MESH)


def meet():
    pl.semaphore_wait(pltpu.get_barrier_semaphore(), 10)


def grant(me, core, credit, phase, axis, direct):
    for i, step in enumerate((RIGHT, LEFT, ACROSS)[:3 if direct else 2]):
        pl.semaphore_signal(credit.at[phase, i], inc=1, device_id=peer(me, core, axis, step), device_id_type=MESH)


def spend(credit, phase, direct):
    for i in range(3 if direct else 2):
        pl.semaphore_wait(credit.at[phase, i], 1)


def tiles(rows, body):
    size = min(rows, 128 if rows % 256 else 256)
    if rows == size:
        body(0, size)
    else:
        @pl.loop(0, rows // size)
        def _(i):
            body(pl.multiple_of(i * size, size), size)


def block_at(me, weights, there):
    at = sum(lax.rem(spot - me[axis] + 4, 4) * weights[axis] for axis, spot in there.items())
    return pl.multiple_of(at * 128, 128)


def pick_tables(blocks, experts, put_pick, put_gain):
    lane = lax.broadcasted_iota(jnp.int32, (128, 128), 1)
    row = lax.broadcasted_iota(jnp.int32, (128, 128), 0)
    before = (row < lane).astype(bf16)
    slot_row = lax.broadcasted_iota(jnp.int32, (80, 256), 0)
    half_lane = lax.broadcasted_iota(jnp.int32, (80, 256), 1)
    second_row, second_lane = slot_row >= 40, half_lane >= 128
    position = jnp.where(second_row, slot_row - 40, slot_row).astype(f32)
    same = second_row == second_lane
    for source, expert in enumerate(experts):
        taken, pos, gain = [], [], []
        for block in blocks:
            block = block.astype(f32)
            code = block[8:16] * 256.0 + block[16:24]
            weight = route_scale * code / jnp.sum(code, axis=0, keepdims=True)
            named = block[0:8] == expert
            hit = jnp.max(jnp.where(named, 1.0, 0.0), axis=0, keepdims=True)
            taken.append(hit)
            wide = jnp.broadcast_to(hit, (8, 128)).astype(bf16)
            pos.append(jnp.dot(wide, before, preferred_element_type=f32)[0:1])
            gain.append(jnp.sum(jnp.where(named, weight, 0.0), axis=0, keepdims=True))
        taken, pos, gain = (jnp.concatenate(v, axis=1) for v in (taken, pos, gain))
        hot = same & (pos == position) & (taken > 0.5)
        put_pick(source, jnp.where(hot, 1.0, 0.0).astype(bf16))
        put_gain(source, jnp.broadcast_to(jnp.sum(jnp.where(hot, gain, 0.0), axis=1, keepdims=True), (80, 128)))


class Gather:
    def __init__(self, me, core, axes, direct, outs, sends, recvs, credit, slots):
        self.me, self.core, self.axes, self.direct, self.outs = me, core, axes, direct, outs
        self.sends, self.recvs, self.credit, self.slots = sends, recvs, credit, slots

    def depth(self, phase):
        return self.outs[phase].shape[0]

    def copy(self, phase, slot, kind):
        p = lax.rem(slot, self.depth(phase))
        buf = self.outs[phase].at[p]
        b = self.outs[phase].shape[1] // 4
        h = b // 2
        src, dst, step = (
            (pl.ds(0, b), pl.ds(3 * b, b), RIGHT),
            (pl.ds(0, b), pl.ds(b, b), LEFT),
            (pl.ds(3 * b, h), pl.ds(2 * b, h), RIGHT),
            (pl.ds(b + h, h), pl.ds(2 * b + h, h), LEFT),
            (pl.ds(0, b), pl.ds(2 * b, b), ACROSS),
        )[4 if self.direct[phase] and kind == 2 else kind]
        return pltpu.make_async_remote_copy(
            src_ref=buf.at[src], dst_ref=buf.at[dst], send_sem=self.sends[phase].at[kind, p], recv_sem=self.recvs[phase].at[kind, p],
            device_id=peer(self.me, self.core, self.axes[phase], step), device_id_type=MESH)

    def begin(self, phase, slot):
        if self.slots > self.depth(phase):
            pl.when(slot >= self.depth(phase))(lambda: spend(self.credit, phase, self.direct[phase]))
        for kind in range(3 if self.direct[phase] else 2):
            self.copy(phase, slot, kind).start()

    def middle(self, phase, slot):
        self.copy(phase, slot, 0).wait_recv()
        self.copy(phase, slot, 2).start()
        self.copy(phase, slot, 1).wait_recv()
        self.copy(phase, slot, 3).start()

    def arrive(self, phase, slot):
        for kind in (0, 1, 2) if self.direct[phase] else (2, 3):
            self.copy(phase, slot, kind).wait_recv()

    def close(self, phase, slot):
        for kind in range(3 if self.direct[phase] else 4):
            self.copy(phase, slot, kind).wait_send()
        if self.slots > self.depth(phase):
            pl.when(slot + self.depth(phase) < self.slots)(
                lambda: grant(self.me, self.core, self.credit, phase, self.axes[phase], self.direct[phase]))

    def forward(self, phase, slot):
        src, dst = self.outs[phase], self.outs[phase + 1]
        p, q = lax.rem(slot, src.shape[0]), lax.rem(slot, dst.shape[0])

        def move(at, n):
            dst[q, pl.ds(at, n), :] = src[p, pl.ds(at, n), :]
        tiles(src.shape[1], move)


def dispatch_kernel(tok_ref, routing_ref, codes_ref, gate_hbm, up_hbm, own_ref, other_ref, pick_ref,
                    gate_ref, up_ref, total, gain_own, gain_send, gain_got, gain_sem, load_sem, credit, *rest):
    rest = list(rest)

    def take(n):
        taken = rest[:n]
        del rest[:n]
        return taken

    me, core = place()
    partner = {"aa": me["z"] * 2 + (1 - core)}
    quarter = tok_ref.shape[1]
    loads = [pltpu.make_async_copy(gate_hbm, gate_ref, load_sem.at[0]), pltpu.make_async_copy(up_hbm, up_ref, load_sem.at[1])]
    greet(me, core)
    for load in loads:
        load.start()
    meet()
    rings, wares = [], []
    for s, (axes, _, slots) in enumerate(STREAMS):
        rings.append(Gather(me, core, axes, (True, False, False), take(3), take(3), take(3), credit.at[s], slots))
        wares.append(take(3 if s < PACKED else 5))
    notes = Gather(me, core, ("x", "z"), (True, True), take(2), take(2), take(2), None, 1)
    gains = pltpu.make_async_remote_copy(
        src_ref=gain_send, dst_ref=gain_got, send_sem=gain_sem.at[0], recv_sem=gain_sem.at[1],
        device_id=partner, device_id_type=MESH)

    def pair(s, slot, part=0):
        if s < PACKED:
            got, send, recv = wares[s]
            b = got.shape[2]
            src = rings[s].outs[2].at[lax.rem(slot, rings[s].depth(2)), pl.ds(2 * b * part + b, b)]
            dst = got.at[lax.rem(slot, 2), part]
            send_at, recv_at = send.at[part], recv.at[lax.rem(slot, 2), part]
        else:
            _, src, got, send, recv = wares[s]
            dst = got.at[lax.rem(slot, 2)]
            send_at, recv_at = send.at[0], recv.at[lax.rem(slot, 2)]
        return pltpu.make_async_remote_copy(
            src_ref=src, dst_ref=dst, send_sem=send_at, recv_sem=recv_at, device_id=partner, device_id_type=MESH)

    def tile_of(s, slot):
        return pl.multiple_of((slot + STREAMS[s][1]) * TILE, TILE)

    def open_tile(s, slot):
        rings[s].outs[0][lax.rem(slot, 2), 0:128, :] = tok_ref[:, pl.ds(tile_of(s, slot), TILE)]
        rings[s].begin(0, slot)

    def pick(n, blocks):
        return jnp.dot(pick_ref[n], jnp.concatenate(blocks, axis=0), preferred_element_type=f32).astype(bf16)

    def pass_on(s, phase, slot):
        ring = rings[s]
        ring.arrive(phase, slot)
        if phase == 1 and s < PACKED:
            src, dst = ring.outs[1], ring.outs[2]
            p, q = lax.rem(slot, ring.depth(1)), lax.rem(slot, ring.depth(2))
            weights = {ring.axes[0]: 1, ring.axes[1]: 4}

            @pl.loop(0, 8)
            def _(n):
                blocks = [src[p, pl.ds(block_at(me, weights, {"z": n // 2, "x": lax.rem(n, 2) * 2 + half}), 128), :] for half in range(2)]
                rows = pick(n, blocks)
                at = pl.multiple_of(n * 80, 16)
                dst[q, pl.ds(at, 80), :] = rows[0:80]
                dst[q, pl.ds(at + 640, 80), :] = rows[80:160]
        else:
            ring.forward(phase, slot)
        ring.begin(phase + 1, slot)
        ring.close(phase, slot)

    def tables():
        experts = [(((me["z"] * 2 + c) * 4) + me["x"]).astype(f32) for c in (core, 1 - core)]

        @pl.loop(0, 8)
        def _(n):
            spots = [block_at(me, {"x": 1, "z": 4}, {"z": n // 2, "x": lax.rem(n, 2) * 2 + half}) // 4 for half in range(2)]
            blocks = [notes.outs[1][0, pl.ds(pl.multiple_of(at, 32), 32), :] for at in spots]

            def put_pick(source, hot):
                pick_ref[n, source * 80:source * 80 + 80, :] = hot

            def put_gain(source, gain):
                (gain_own, gain_send)[source][n] = gain
            pick_tables(blocks, experts, put_pick, put_gain)
        gains.start()

    def collect(s, slot):
        ring = rings[s]
        ring.arrive(2, slot)
        if s < PACKED:
            for part in range(4):
                pair(s, slot, part).start()
            return
        own, send = wares[s][:2]
        p = lax.rem(slot, ring.depth(2))
        weights = {axis: 4 ** i for i, axis in enumerate(ring.axes)}
        pl.when(slot >= 1)(lambda: pair(s, slot - 1).wait_send())

        @pl.loop(0, 8)
        def _(n):
            blocks = [jnp.concatenate([ring.outs[2][p, pl.ds(block_at(me, weights, {"z": n // 2, "x": lax.rem(n, 2) * 2 + half, "y": q}), 128), :]
                                       for q in range(4)], axis=1) for half in range(2)]
            rows = pick(n, blocks)
            at = pl.ds(pl.multiple_of(n * 80, 16), 80)
            own[at, :] = rows[0:80]
            send[at, :] = rows[80:160]
        pair(s, slot).start()
        pl.when(slot == ring.slots - 1)(lambda: pair(s, slot).wait_send())
        ring.close(2, slot)

    def multiply(s, slot):
        ring = rings[s]
        first = tile_of(s, slot)
        if s < PACKED:
            for part in range(4):
                pair(s, slot, part).wait_recv()
            got = wares[s][0]
            quarters = [lax.rem(me["y"] + part, 4) for part in range(4)]
            p = lax.rem(slot, ring.depth(2))
            rows = (jnp.concatenate([ring.outs[2][p, pl.ds(1280 * part, 640), :] for part in range(4)], axis=1),
                    jnp.concatenate([got[lax.rem(slot, 2), part] for part in range(4)], axis=1))
        else:
            pair(s, slot).wait_recv()
            quarters = range(4)
            rows = (wares[s][0][...], wares[s][2][lax.rem(slot, 2)])
        for w_ref, col in ((gate_ref, 0), (up_ref, 512)):
            w = jnp.concatenate([w_ref[pl.ds(pl.multiple_of(q * quarter + first, TILE), TILE), :] for q in quarters], axis=0)
            for half in range(2):
                total[half, :, col:col + 512] += jnp.dot(rows[half], w, preferred_element_type=f32)
        if s < PACKED:
            for part in range(4):
                pair(s, slot, part).wait_send()
            ring.close(2, slot)

    def stage(step, delay, body):
        for s, (_, _, slots) in enumerate(STREAMS):
            slot = step - delay
            pl.when((slot >= 0) & (slot < slots))(functools.partial(body, s, slot))

    def note(step, at, body):
        pl.when(step == at)(body)

    def note_open():
        codes = codes_ref[...].astype(f32)
        high = jnp.floor(codes * (1.0 / 256.0))
        notes.outs[0][0, 0:32, :] = jnp.concatenate(
            [routing_ref[...].astype(f32), high, codes - 256.0 * high, jnp.zeros((8, 128), f32)], axis=0).astype(bf16)
        notes.begin(0, 0)

    def note_pass():
        notes.arrive(0, 0)
        notes.forward(0, 0)
        notes.begin(1, 0)
        notes.close(0, 0)

    def note_end():
        notes.arrive(1, 0)
        tables()
        notes.close(1, 0)

    def consume(step):
        def one(s, body):
            slot = step - 5
            pl.when((slot >= 0) & (slot < STREAMS[s][2]))(lambda: body(s, slot))

        for s in range(len(STREAMS)):
            one(s, collect)
        for s in range(len(STREAMS)):
            one(s, multiply)

    @pl.loop(0, max(slots for _, _, slots in STREAMS) + 5)
    def _(step):
        note(step, 1, note_pass)
        note(step, 0, note_open)
        stage(step, 4, lambda s, slot: rings[s].middle(2, slot))
        stage(step, 3, lambda s, slot: pass_on(s, 1, slot))
        stage(step, 2, lambda s, slot: rings[s].middle(1, slot))
        stage(step, 1, lambda s, slot: pass_on(s, 0, slot))
        stage(step, 0, open_tile)
        note(step, 2, note_end)

        @pl.when(step == 1)
        def _():
            total[...] = jnp.zeros_like(total)

        @pl.when(step == 4)
        def _():
            for load in loads:
                load.wait()

        consume(step)

    gains.wait()

    @pl.loop(0, 8)
    def _(n):
        at = pl.ds(pl.multiple_of(n * 80, 16), 80)
        for half, ref, gain in ((0, own_ref, gain_own), (1, other_ref, gain_got)):
            gate = total[half, at, 0:512]
            upper = total[half, at, 512:1024]
            ref[at, :] = (jax.nn.silu(gate) * upper * gain[n][:, 0:1]).astype(bf16)


def rows_buffer(*shape):
    return pltpu.VMEM(shape + (TILE,), bf16)


def dispatch(tokens, routing, codes, gate, up):
    vmem = pl.BlockSpec(memory_space=pltpu.VMEM)
    hbm = pl.BlockSpec(memory_space=pl.ANY)
    dma = pltpu.SemaphoreType.DMA
    hidden = jax.ShapeDtypeStruct((640, 512), bf16)
    scratch = [
        pltpu.VMEM(gate.shape, bf16), pltpu.VMEM(up.shape, bf16), pltpu.VMEM((2, 640, 1024), f32),
        pltpu.VMEM((8, 80, 128), f32), pltpu.VMEM((8, 80, 128), f32), pltpu.VMEM((8, 80, 128), f32),
        dma((2,)), dma((2,)), pltpu.SemaphoreType.REGULAR((len(STREAMS), 3, 3)),
    ]
    for s in range(len(STREAMS)):
        scratch += [rows_buffer(2, 512), rows_buffer(3, 2048), rows_buffer(3, 5120 if s < PACKED else 8192)]
        scratch += [dma((4, 2)), dma((4, 3)), dma((4, 3))] * 2
        if s < PACKED:
            scratch += [rows_buffer(2, 4, 640), dma((4,)), dma((2, 4))]
        else:
            scratch += [pltpu.VMEM((640, 512), bf16), pltpu.VMEM((640, 512), bf16), pltpu.VMEM((2, 640, 512), bf16), dma((1,)), dma((2,))]
    scratch += [rows_buffer(1, 128), rows_buffer(1, 512)] + [dma((4, 1))] * 4
    return pl.pallas_call(
        dispatch_kernel,
        out_shape=(hidden, hidden, jax.ShapeDtypeStruct((8, 160, 256), bf16)),
        in_specs=[vmem, vmem, vmem, hbm, hbm],
        out_specs=(vmem,) * 3,
        scratch_shapes=scratch,
        compiler_params=pltpu.CompilerParams(collective_id=0, has_side_effects=True, vmem_limit_bytes=66900000),
        name="dispatch",
    )(tokens, routing, codes, gate, up)


class Reduce:
    def __init__(self, me, core, axes, direct, ins, gots, mores, sends, recvs, credit, slots):
        self.me, self.core, self.axes, self.direct = me, core, axes, direct
        self.ins, self.gots, self.mores = ins, gots, mores
        self.sends, self.recvs, self.credit, self.slots = sends, recvs, credit, slots

    def depth(self, phase):
        return self.ins[phase].shape[0]

    def copy(self, phase, slot, kind):
        p = lax.rem(slot, self.depth(phase))
        buf = self.ins[phase].at[p]
        b = self.ins[phase].shape[1] // 4
        h = b // 2
        got, more = self.gots[phase], self.mores[phase]
        if self.direct[phase]:
            src, dst, step = (
                (pl.ds(b, b), got.at[p, 0], RIGHT),
                (pl.ds(3 * b, b), got.at[p, 1], LEFT),
                (pl.ds(2 * b, b), more.at[p, 0], ACROSS),
            )[kind]
        else:
            src, dst, step = (
                (pl.ds(b + h, b), got.at[p, 0], RIGHT),
                (pl.ds(2 * b + h, b), got.at[p, 1], LEFT),
                (pl.ds(b, h), more.at[p, 0], RIGHT),
                (pl.ds(3 * b + h, h), more.at[p, 1], LEFT),
            )[kind]
        return pltpu.make_async_remote_copy(
            src_ref=buf.at[src], dst_ref=dst, send_sem=self.sends[phase].at[kind, p], recv_sem=self.recvs[phase].at[kind, p],
            device_id=peer(self.me, self.core, self.axes[phase], step), device_id_type=MESH)

    def begin(self, phase, slot):
        if self.slots > self.depth(phase):
            pl.when(slot >= self.depth(phase))(lambda: spend(self.credit, phase, self.direct[phase]))
        for kind in range(3 if self.direct[phase] else 2):
            self.copy(phase, slot, kind).start()

    def middle(self, phase, slot):
        p = lax.rem(slot, self.depth(phase))
        buf, got = self.ins[phase], self.gots[phase]
        b = buf.shape[1] // 4
        h = b // 2
        for kind, base, skip in ((0, b, h), (1, 3 * b + h, 0)):
            self.copy(phase, slot, kind).wait_recv()

            def add(i, n):
                at = pl.ds(base + i, n)
                buf[p, at, :] = (buf[p, at, :].astype(f32) + got[p, kind, pl.ds(skip + i, n), :].astype(f32)).astype(bf16)
            tiles(h, add)
            self.copy(phase, slot, kind + 2).start()

    def finish(self, phase, slot, put):
        p = lax.rem(slot, self.depth(phase))
        buf, got, more = self.ins[phase], self.gots[phase], self.mores[phase]
        b = buf.shape[1] // 4
        h = b // 2
        if self.direct[phase]:
            for kind in range(3):
                self.copy(phase, slot, kind).wait_recv()

            def add_all(at, n):
                value = ((buf[p, pl.ds(at, n), :].astype(f32) + got[p, 0, pl.ds(at, n), :].astype(f32))
                         + (got[p, 1, pl.ds(at, n), :].astype(f32) + more[p, 0, pl.ds(at, n), :].astype(f32)))
                put(at, n, value.astype(bf16))
            tiles(b, add_all)
            return
        for kind, base, skip in ((0, 0, h), (1, h, 0)):
            self.copy(phase, slot, kind + 2).wait_recv()

            def add(i, n):
                at = base + i
                value = (buf[p, pl.ds(at, n), :].astype(f32) + got[p, 1 - kind, pl.ds(skip + i, n), :].astype(f32)
                         + more[p, kind, pl.ds(i, n), :].astype(f32))
                put(at, n, value.astype(bf16))
            tiles(h, add)

    def close(self, phase, slot):
        for kind in range(3 if self.direct[phase] else 4):
            self.copy(phase, slot, kind).wait_send()
        if self.slots > self.depth(phase):
            pl.when(slot + self.depth(phase) < self.slots)(
                lambda: grant(self.me, self.core, self.credit, phase, self.axes[phase], self.direct[phase]))


def combine_kernel(own_ref, other_ref, down_hbm, pick_ref, out_ref, down_ref, load_sem, credit, *rest):
    rest = list(rest)

    def take(n):
        taken = rest[:n]
        del rest[:n]
        return taken

    me, core = place()
    partner = {"aa": me["z"] * 2 + (1 - core)}
    quarter = out_ref.shape[1]
    order = (0, 1, 2, 3)

    def load(s, slot, part):
        q = lax.rem(me["y"] + part, 4) if s < PACKED else part
        at = slot + STREAMS[s][1]
        return pltpu.make_async_copy(
            down_hbm.at[:, pl.ds(pl.multiple_of(q * quarter + at * TILE, TILE), TILE)],
            down_ref.at[at, :, pl.ds(part * TILE, TILE)], load_sem.at[at, part])

    greet(me, core)
    for slot in range(max(slots for _, _, slots in STREAMS)):
        for s in order:
            if slot < STREAMS[s][2]:
                for part in range(4):
                    load(s, slot, part).start()
    meet()
    rings, wares = [], []
    for s, (axes, _, slots) in enumerate(STREAMS):
        rings.append(Reduce(me, core, axes[::-1], (False, False, True), take(3), take(3), take(3), take(3), take(3), credit.at[s], slots))
        wares.append(take(6 if s < PACKED else 4))

    def pair(s, slot):
        p = lax.rem(slot, 2)
        if s < PACKED:
            _, src, got, _, send, recv = wares[s]
            dst = got.at[p]
        else:
            src, got, send, recv = wares[s]
            dst = got.at[p, :, pl.ds(80, 80)]
        return pltpu.make_async_remote_copy(
            src_ref=src, dst_ref=dst, send_sem=send.at[0], recv_sem=recv.at[p], device_id=partner, device_id_type=MESH)

    def tile_of(s, slot):
        return pl.multiple_of((slot + STREAMS[s][1]) * TILE, TILE)

    def project(s, slot):
        for part in range(4):
            load(s, slot, part).wait()
        w = down_ref[slot + STREAMS[s][1]]
        mine = jnp.dot(own_ref[...], w, preferred_element_type=f32).astype(bf16)
        if s < PACKED:
            for part in range(4):
                wares[s][0][part] = mine[:, part * TILE:(part + 1) * TILE]
        else:
            wares[s][1][lax.rem(slot, 2), :, 0:80, :] = mine.reshape(8, 80, 4 * TILE)
        pl.when(slot >= 1)(lambda: pair(s, slot - 1).wait_send())
        theirs = jnp.dot(other_ref[...], w, preferred_element_type=f32).astype(bf16)
        if s < PACKED:
            for part in range(4):
                wares[s][1][part] = theirs[:, part * TILE:(part + 1) * TILE]
        else:
            wares[s][0][...] = theirs.reshape(8, 80, 4 * TILE)
        pair(s, slot).start()
        pl.when(slot == rings[s].slots - 1)(lambda: pair(s, slot).wait_send())

    def spread(n, rows):
        return lax.dot_general(pick_ref[n], rows, (((0,), (0,)), ((), ())), preferred_element_type=f32).astype(bf16)

    def launch(s, slot):
        ring = rings[s]
        p, d = lax.rem(slot, ring.depth(0)), lax.rem(slot, 2)
        first_in = ring.ins[0]
        pair(s, slot).wait_recv()
        if s < PACKED:
            own, _, got = wares[s][:3]

            @pl.loop(0, 4)
            def _(part):
                at = pl.multiple_of(part * 1280, 1280)
                first_in[p, pl.ds(at, 640), :] = own[part]
                first_in[p, pl.ds(at + 640, 640), :] = got[d, part]
        else:
            weights = {axis: 4 ** (2 - i) for i, axis in enumerate(ring.axes)}

            @pl.loop(0, 8)
            def _(n):
                rows = spread(n, wares[s][1][d, n])
                for half in range(2):
                    for q in range(4):
                        at = block_at(me, weights, {"z": n // 2, "x": lax.rem(n, 2) * 2 + half, "y": q})
                        first_in[p, pl.ds(at, 128), :] = rows[half * 128:half * 128 + 128, q * TILE:(q + 1) * TILE]
        ring.begin(0, slot)

    def pass_on(s, phase, slot):
        ring = rings[s]
        dst, p = ring.ins[phase + 1], lax.rem(slot, 2)
        if phase == 0 and s < PACKED:
            summed = wares[s][3]

            def hold(at, n, value):
                summed[pl.ds(at, n), :] = value
            ring.finish(0, slot, hold)
            weights = {ring.axes[1]: 4, ring.axes[2]: 1}

            @pl.loop(0, 8)
            def _(n):
                at = pl.multiple_of(n * 80, 16)
                rows = spread(n, jnp.concatenate([summed[pl.ds(at, 80), :], summed[pl.ds(at + 640, 80), :]], axis=0))
                for half in range(2):
                    at = block_at(me, weights, {"z": n // 2, "x": lax.rem(n, 2) * 2 + half})
                    dst[p, pl.ds(at, 128), :] = rows[half * 128:half * 128 + 128]
        else:
            def put(at, n, value):
                dst[p, pl.ds(at, n), :] = value
            ring.finish(phase, slot, put)
        ring.begin(phase + 1, slot)
        ring.close(phase, slot)

    def deliver(s, slot):
        def put(at, n, value):
            out_ref[pl.ds(at, n), pl.ds(tile_of(s, slot), TILE)] = value
        rings[s].finish(2, slot, put)
        rings[s].close(2, slot)

    def stage(step, delay, body, lowest=0, streams=range(len(STREAMS))):
        for s in streams:
            slot = step - delay
            pl.when((slot >= lowest) & (slot < STREAMS[s][2]))(functools.partial(body, s, slot))

    start = jnp.int32(0)
    project(order[0], start)
    for before, s in zip(order, order[1:]):
        project(s, start)
        launch(before, start)
    launch(order[-1], start)
    packed, plain = range(PACKED), range(PACKED, len(STREAMS))

    @pl.loop(0, max(slots for _, _, slots in STREAMS) + 5)
    def _(step):
        stage(step, 1, lambda s, slot: rings[s].middle(0, slot))
        stage(step, 0, launch, 1, packed)
        stage(step, 3, lambda s, slot: rings[s].middle(1, slot))
        stage(step, 5, deliver)
        stage(step, 4, lambda s, slot: pass_on(s, 1, slot))
        for s in plain:
            stage(step, 2, lambda s, slot: pass_on(s, 0, slot), 0, (s,))
            stage(step, 0, launch, 1, (s,))
        stage(step, 2, lambda s, slot: pass_on(s, 0, slot), 0, packed)
        stage(step, -1, project, 1)


def combine(own, other, down, pick):
    quarter = down.shape[1] // 4
    vmem = pl.BlockSpec(memory_space=pltpu.VMEM)
    dma = pltpu.SemaphoreType.DMA
    count = quarter // TILE
    scratch = [pltpu.VMEM((count, down.shape[0], 4 * TILE), bf16), dma((count, 4)), pltpu.SemaphoreType.REGULAR((len(STREAMS), 3, 3))]
    for s in range(len(STREAMS)):
        sizes = (5120 if s < PACKED else 8192, 2048, 512)
        depths = (3 if s < PACKED else 2, 2, 2)
        scratch += [rows_buffer(d, n) for d, n in zip(depths, sizes)]
        scratch += [rows_buffer(d, 2, n // 4) for d, n in zip(depths, sizes)]
        scratch += [rows_buffer(depths[0], 2, sizes[0] // 8), rows_buffer(2, 2, sizes[1] // 8), rows_buffer(2, 1, sizes[2] // 4)]
        scratch += [dma((4, d)) for d in depths] * 2
        if s < PACKED:
            scratch += [rows_buffer(4, 640), rows_buffer(4, 640), rows_buffer(2, 4, 640), rows_buffer(1280), dma((1,)), dma((2,))]
        else:
            scratch += [pltpu.VMEM((8, 80, 512), bf16), pltpu.VMEM((2, 8, 160, 512), bf16), dma((1,)), dma((2,))]
    return pl.pallas_call(
        combine_kernel,
        out_shape=jax.ShapeDtypeStruct((128, quarter), bf16),
        in_specs=[vmem, vmem, pl.BlockSpec(memory_space=pl.ANY), vmem],
        out_specs=vmem,
        scratch_shapes=scratch,
        compiler_params=pltpu.CompilerParams(collective_id=1, has_side_effects=True, vmem_limit_bytes=66900000),
        name="combine",
    )(own, other, down, pick)


def on_device(tokens, routing, gate_codes, w_gate, w_up, w_down):
    own, other, pick = dispatch(tokens, routing.T, gate_codes.T, w_gate[0], w_up[0])
    return combine(own, other, w_down[0], pick)


def solution(mesh):
    return jax.shard_map(
        on_device,
        mesh=mesh,
        in_specs=(
            P(("aa", "col"), "ba"),
            P(("aa", "col"), None),
            P(("aa", "col"), None),
            P(("aa", "col"), None, "ba"),
            P(("aa", "col"), None, "ba"),
            P(("aa", "col"), "ba", None),
        ),
        out_specs=P(("aa", "col"), "ba"),
        check_vma=False,
    )
```

```python
import functools
import jax
import jax.numpy as jnp
from jax import lax
from jax.experimental import pallas as pl
from jax.experimental.pallas import tpu as pltpu
from jax.sharding import PartitionSpec as P

MESH = pl.DeviceIdType.MESH
route_scale = 2.827
bf16 = jnp.bfloat16
f32 = jnp.float32
TILE = 128
STREAMS = ((("z", "x", "y"), 0, 4), (("x", "z", "y"), 4, 4), (("y", "z", "x"), 8, 3), (("y", "x", "z"), 11, 3))
PACKED = 2
RIGHT, LEFT, ACROSS = 1, -1, 2


def place():
    aa = lax.axis_index("aa")
    return {"z": aa // 2, "y": lax.axis_index("ba"), "x": lax.axis_index("col")}, aa % 2


def peer(me, core, axis, step):
    at = lax.rem(me[axis] + (step + 4), 4)
    if axis == "z":
        return {"aa": at * 2 + core}
    return {"ba": at} if axis == "y" else {"col": at}


def greet(me, core):
    barrier = pltpu.get_barrier_semaphore()
    for axis in "xyz":
        for step in (RIGHT, LEFT, ACROSS):
            pl.semaphore_signal(barrier, inc=1, device_id=peer(me, core, axis, step), device_id_type=MESH)
    pl.semaphore_signal(barrier, inc=1, device_id={"aa": me["z"] * 2 + (1 - core)}, device_id_type=MESH)


def meet():
    pl.semaphore_wait(pltpu.get_barrier_semaphore(), 10)


def grant(me, core, credit, phase, axis, direct):
    for i, step in enumerate((RIGHT, LEFT, ACROSS)[:3 if direct else 2]):
        pl.semaphore_signal(credit.at[phase, i], inc=1, device_id=peer(me, core, axis, step), device_id_type=MESH)


def spend(credit, phase, direct):
    for i in range(3 if direct else 2):
        pl.semaphore_wait(credit.at[phase, i], 1)


def tiles(rows, body):
    size = min(rows, 128 if rows % 256 else 256)
    if rows == size:
        body(0, size)
    else:
        @pl.loop(0, rows // size)
        def _(i):
            body(pl.multiple_of(i * size, size), size)


def block_at(me, weights, there):
    at = sum(lax.rem(spot - me[axis] + 4, 4) * weights[axis] for axis, spot in there.items())
    return pl.multiple_of(at * 128, 128)


def pick_tables(blocks, experts, put_pick, put_gain):
    lane = lax.broadcasted_iota(jnp.int32, (128, 128), 1)
    row = lax.broadcasted_iota(jnp.int32, (128, 128), 0)
    before = (row < lane).astype(bf16)
    slot_row = lax.broadcasted_iota(jnp.int32, (80, 256), 0)
    half_lane = lax.broadcasted_iota(jnp.int32, (80, 256), 1)
    second_row, second_lane = slot_row >= 40, half_lane >= 128
    position = jnp.where(second_row, slot_row - 40, slot_row).astype(f32)
    same = second_row == second_lane
    for source, expert in enumerate(experts):
        taken, pos, gain = [], [], []
        for block in blocks:
            block = block.astype(f32)
            code = block[8:16] * 256.0 + block[16:24]
            weight = route_scale * code / jnp.sum(code, axis=0, keepdims=True)
            named = block[0:8] == expert
            hit = jnp.max(jnp.where(named, 1.0, 0.0), axis=0, keepdims=True)
            taken.append(hit)
            wide = jnp.broadcast_to(hit, (8, 128)).astype(bf16)
            pos.append(jnp.dot(wide, before, preferred_element_type=f32)[0:1])
            gain.append(jnp.sum(jnp.where(named, weight, 0.0), axis=0, keepdims=True))
        taken, pos, gain = (jnp.concatenate(v, axis=1) for v in (taken, pos, gain))
        hot = same & (pos == position) & (taken > 0.5)
        put_pick(source, jnp.where(hot, 1.0, 0.0).astype(bf16))
        put_gain(source, jnp.broadcast_to(jnp.sum(jnp.where(hot, gain, 0.0), axis=1, keepdims=True), (80, 128)))


class Gather:
    def __init__(self, me, core, axes, direct, outs, sends, recvs, credit, slots):
        self.me, self.core, self.axes, self.direct, self.outs = me, core, axes, direct, outs
        self.sends, self.recvs, self.credit, self.slots = sends, recvs, credit, slots

    def depth(self, phase):
        return self.outs[phase].shape[0]

    def copy(self, phase, slot, kind):
        p = lax.rem(slot, self.depth(phase))
        buf = self.outs[phase].at[p]
        b = self.outs[phase].shape[1] // 4
        h = b // 2
        src, dst, step = (
            (pl.ds(0, b), pl.ds(3 * b, b), RIGHT),
            (pl.ds(0, b), pl.ds(b, b), LEFT),
            (pl.ds(3 * b, h), pl.ds(2 * b, h), RIGHT),
            (pl.ds(b + h, h), pl.ds(2 * b + h, h), LEFT),
            (pl.ds(0, b), pl.ds(2 * b, b), ACROSS),
        )[4 if self.direct[phase] and kind == 2 else kind]
        return pltpu.make_async_remote_copy(
            src_ref=buf.at[src], dst_ref=buf.at[dst], send_sem=self.sends[phase].at[kind, p], recv_sem=self.recvs[phase].at[kind, p],
            device_id=peer(self.me, self.core, self.axes[phase], step), device_id_type=MESH)

    def begin(self, phase, slot):
        if self.slots > self.depth(phase):
            pl.when(slot >= self.depth(phase))(lambda: spend(self.credit, phase, self.direct[phase]))
        for kind in range(3 if self.direct[phase] else 2):
            self.copy(phase, slot, kind).start()

    def middle(self, phase, slot):
        self.copy(phase, slot, 0).wait_recv()
        self.copy(phase, slot, 2).start()
        self.copy(phase, slot, 1).wait_recv()
        self.copy(phase, slot, 3).start()

    def arrive(self, phase, slot):
        for kind in (0, 1, 2) if self.direct[phase] else (2, 3):
            self.copy(phase, slot, kind).wait_recv()

    def close(self, phase, slot):
        for kind in range(3 if self.direct[phase] else 4):
            self.copy(phase, slot, kind).wait_send()
        if self.slots > self.depth(phase):
            pl.when(slot + self.depth(phase) < self.slots)(
                lambda: grant(self.me, self.core, self.credit, phase, self.axes[phase], self.direct[phase]))

    def forward(self, phase, slot):
        src, dst = self.outs[phase], self.outs[phase + 1]
        p, q = lax.rem(slot, src.shape[0]), lax.rem(slot, dst.shape[0])

        def move(at, n):
            dst[q, pl.ds(at, n), :] = src[p, pl.ds(at, n), :]
        tiles(src.shape[1], move)


def dispatch_kernel(tok_ref, routing_ref, codes_ref, gate_hbm, up_hbm, own_ref, other_ref, pick_ref,
                    gate_ref, up_ref, total, gain_own, gain_send, gain_got, gain_sem, load_sem, credit, *rest):
    rest = list(rest)

    def take(n):
        taken = rest[:n]
        del rest[:n]
        return taken

    me, core = place()
    partner = {"aa": me["z"] * 2 + (1 - core)}
    quarter = tok_ref.shape[1]
    loads = [pltpu.make_async_copy(gate_hbm, gate_ref, load_sem.at[0]), pltpu.make_async_copy(up_hbm, up_ref, load_sem.at[1])]
    greet(me, core)
    for load in loads:
        load.start()
    meet()
    rings, wares = [], []
    for s, (axes, _, slots) in enumerate(STREAMS):
        rings.append(Gather(me, core, axes, (True, False, False), take(3), take(3), take(3), credit.at[s], slots))
        wares.append(take(3 if s < PACKED else 5))
    notes = Gather(me, core, ("x", "z"), (True, True), take(2), take(2), take(2), None, 1)
    gains = pltpu.make_async_remote_copy(
        src_ref=gain_send, dst_ref=gain_got, send_sem=gain_sem.at[0], recv_sem=gain_sem.at[1],
        device_id=partner, device_id_type=MESH)

    def pair(s, slot, part=0):
        if s < PACKED:
            got, send, recv = wares[s]
            b = got.shape[2]
            src = rings[s].outs[2].at[lax.rem(slot, rings[s].depth(2)), pl.ds(2 * b * part + b, b)]
            dst = got.at[lax.rem(slot, 2), part]
            send_at, recv_at = send.at[part], recv.at[lax.rem(slot, 2), part]
        else:
            _, src, got, send, recv = wares[s]
            dst = got.at[lax.rem(slot, 2)]
            send_at, recv_at = send.at[0], recv.at[lax.rem(slot, 2)]
        return pltpu.make_async_remote_copy(
            src_ref=src, dst_ref=dst, send_sem=send_at, recv_sem=recv_at, device_id=partner, device_id_type=MESH)

    def tile_of(s, slot):
        return pl.multiple_of((slot + STREAMS[s][1]) * TILE, TILE)

    def open_tile(s, slot):
        rings[s].outs[0][lax.rem(slot, 2), 0:128, :] = tok_ref[:, pl.ds(tile_of(s, slot), TILE)]
        rings[s].begin(0, slot)

    def pick(n, blocks):
        return jnp.dot(pick_ref[n], jnp.concatenate(blocks, axis=0), preferred_element_type=f32).astype(bf16)

    def pass_on(s, phase, slot):
        ring = rings[s]
        ring.arrive(phase, slot)
        if phase == 1 and s < PACKED:
            src, dst = ring.outs[1], ring.outs[2]
            p, q = lax.rem(slot, ring.depth(1)), lax.rem(slot, ring.depth(2))
            weights = {ring.axes[0]: 1, ring.axes[1]: 4}

            @pl.loop(0, 8)
            def _(n):
                blocks = [src[p, pl.ds(block_at(me, weights, {"z": n // 2, "x": lax.rem(n, 2) * 2 + half}), 128), :] for half in range(2)]
                rows = pick(n, blocks)
                at = pl.multiple_of(n * 80, 16)
                dst[q, pl.ds(at, 80), :] = rows[0:80]
                dst[q, pl.ds(at + 640, 80), :] = rows[80:160]
        else:
            ring.forward(phase, slot)
        ring.begin(phase + 1, slot)
        ring.close(phase, slot)

    def tables():
        experts = [(((me["z"] * 2 + c) * 4) + me["x"]).astype(f32) for c in (core, 1 - core)]

        @pl.loop(0, 8)
        def _(n):
            spots = [block_at(me, {"x": 1, "z": 4}, {"z": n // 2, "x": lax.rem(n, 2) * 2 + half}) // 4 for half in range(2)]
            blocks = [notes.outs[1][0, pl.ds(pl.multiple_of(at, 32), 32), :] for at in spots]

            def put_pick(source, hot):
                pick_ref[n, source * 80:source * 80 + 80, :] = hot

            def put_gain(source, gain):
                (gain_own, gain_send)[source][n] = gain
            pick_tables(blocks, experts, put_pick, put_gain)
        gains.start()

    def collect(s, slot):
        ring = rings[s]
        ring.arrive(2, slot)
        if s < PACKED:
            for part in range(4):
                pair(s, slot, part).start()
            return
        own, send = wares[s][:2]
        p = lax.rem(slot, ring.depth(2))
        weights = {axis: 4 ** i for i, axis in enumerate(ring.axes)}
        pl.when(slot >= 1)(lambda: pair(s, slot - 1).wait_send())

        @pl.loop(0, 8)
        def _(n):
            blocks = [jnp.concatenate([ring.outs[2][p, pl.ds(block_at(me, weights, {"z": n // 2, "x": lax.rem(n, 2) * 2 + half, "y": q}), 128), :]
                                       for q in range(4)], axis=1) for half in range(2)]
            rows = pick(n, blocks)
            at = pl.ds(pl.multiple_of(n * 80, 16), 80)
            own[at, :] = rows[0:80]
            send[at, :] = rows[80:160]
        pair(s, slot).start()
        pl.when(slot == ring.slots - 1)(lambda: pair(s, slot).wait_send())
        ring.close(2, slot)

    def multiply(s, slot):
        ring = rings[s]
        first = tile_of(s, slot)
        if s < PACKED:
            for part in range(4):
                pair(s, slot, part).wait_recv()
            got = wares[s][0]
            quarters = [lax.rem(me["y"] + part, 4) for part in range(4)]
            p = lax.rem(slot, ring.depth(2))
            rows = (jnp.concatenate([ring.outs[2][p, pl.ds(1280 * part, 640), :] for part in range(4)], axis=1),
                    jnp.concatenate([got[lax.rem(slot, 2), part] for part in range(4)], axis=1))
        else:
            pair(s, slot).wait_recv()
            quarters = range(4)
            rows = (wares[s][0][...], wares[s][2][lax.rem(slot, 2)])
        for w_ref, col in ((gate_ref, 0), (up_ref, 512)):
            w = jnp.concatenate([w_ref[pl.ds(pl.multiple_of(q * quarter + first, TILE), TILE), :] for q in quarters], axis=0)
            for half in range(2):
                total[half, :, col:col + 512] += jnp.dot(rows[half], w, preferred_element_type=f32)
        if s < PACKED:
            for part in range(4):
                pair(s, slot, part).wait_send()
            ring.close(2, slot)

    def stage(step, delay, body):
        for s, (_, _, slots) in enumerate(STREAMS):
            slot = step - delay
            pl.when((slot >= 0) & (slot < slots))(functools.partial(body, s, slot))

    def note(step, at, body):
        pl.when(step == at)(body)

    def note_open():
        codes = codes_ref[...].astype(f32)
        high = jnp.floor(codes * (1.0 / 256.0))
        notes.outs[0][0, 0:32, :] = jnp.concatenate(
            [routing_ref[...].astype(f32), high, codes - 256.0 * high, jnp.zeros((8, 128), f32)], axis=0).astype(bf16)
        notes.begin(0, 0)

    def note_pass():
        notes.arrive(0, 0)
        notes.forward(0, 0)
        notes.begin(1, 0)
        notes.close(0, 0)

    def note_end():
        notes.arrive(1, 0)
        tables()
        notes.close(1, 0)

    def consume(step):
        def one(s, body):
            slot = step - 5
            pl.when((slot >= 0) & (slot < STREAMS[s][2]))(lambda: body(s, slot))

        for s in range(len(STREAMS)):
            one(s, collect)
        for s in range(len(STREAMS)):
            one(s, multiply)

    @pl.loop(0, max(slots for _, _, slots in STREAMS) + 5)
    def _(step):
        note(step, 1, note_pass)
        note(step, 0, note_open)
        stage(step, 4, lambda s, slot: rings[s].middle(2, slot))
        stage(step, 3, lambda s, slot: pass_on(s, 1, slot))
        stage(step, 2, lambda s, slot: rings[s].middle(1, slot))
        stage(step, 1, lambda s, slot: pass_on(s, 0, slot))
        stage(step, 0, open_tile)
        note(step, 2, note_end)

        @pl.when(step == 1)
        def _():
            total[...] = jnp.zeros_like(total)

        @pl.when(step == 4)
        def _():
            for load in loads:
                load.wait()

        consume(step)

    gains.wait()

    @pl.loop(0, 8)
    def _(n):
        at = pl.ds(pl.multiple_of(n * 80, 16), 80)
        for half, ref, gain in ((0, own_ref, gain_own), (1, other_ref, gain_got)):
            gate = total[half, at, 0:512]
            upper = total[half, at, 512:1024]
            ref[at, :] = (jax.nn.silu(gate) * upper * gain[n][:, 0:1]).astype(bf16)


def rows_buffer(*shape):
    return pltpu.VMEM(shape + (TILE,), bf16)


def dispatch(tokens, routing, codes, gate, up):
    vmem = pl.BlockSpec(memory_space=pltpu.VMEM)
    hbm = pl.BlockSpec(memory_space=pl.ANY)
    dma = pltpu.SemaphoreType.DMA
    hidden = jax.ShapeDtypeStruct((640, 512), bf16)
    scratch = [
        pltpu.VMEM(gate.shape, bf16), pltpu.VMEM(up.shape, bf16), pltpu.VMEM((2, 640, 1024), f32),
        pltpu.VMEM((8, 80, 128), f32), pltpu.VMEM((8, 80, 128), f32), pltpu.VMEM((8, 80, 128), f32),
        dma((2,)), dma((2,)), pltpu.SemaphoreType.REGULAR((len(STREAMS), 3, 3)),
    ]
    for s in range(len(STREAMS)):
        scratch += [rows_buffer(2, 512), rows_buffer(3, 2048), rows_buffer(3, 5120 if s < PACKED else 8192)]
        scratch += [dma((4, 2)), dma((4, 3)), dma((4, 3))] * 2
        if s < PACKED:
            scratch += [rows_buffer(2, 4, 640), dma((4,)), dma((2, 4))]
        else:
            scratch += [pltpu.VMEM((640, 512), bf16), pltpu.VMEM((640, 512), bf16), pltpu.VMEM((2, 640, 512), bf16), dma((1,)), dma((2,))]
    scratch += [rows_buffer(1, 128), rows_buffer(1, 512)] + [dma((4, 1))] * 4
    return pl.pallas_call(
        dispatch_kernel,
        out_shape=(hidden, hidden, jax.ShapeDtypeStruct((8, 160, 256), bf16)),
        in_specs=[vmem, vmem, vmem, hbm, hbm],
        out_specs=(vmem,) * 3,
        scratch_shapes=scratch,
        compiler_params=pltpu.CompilerParams(collective_id=0, has_side_effects=True, vmem_limit_bytes=66900000),
        name="dispatch",
    )(tokens, routing, codes, gate, up)


class Reduce:
    def __init__(self, me, core, axes, direct, ins, gots, mores, sends, recvs, credit, slots):
        self.me, self.core, self.axes, self.direct = me, core, axes, direct
        self.ins, self.gots, self.mores = ins, gots, mores
        self.sends, self.recvs, self.credit, self.slots = sends, recvs, credit, slots

    def depth(self, phase):
        return self.ins[phase].shape[0]

    def copy(self, phase, slot, kind):
        p = lax.rem(slot, self.depth(phase))
        buf = self.ins[phase].at[p]
        b = self.ins[phase].shape[1] // 4
        h = b // 2
        got, more = self.gots[phase], self.mores[phase]
        if self.direct[phase]:
            src, dst, step = (
                (pl.ds(b, b), got.at[p, 0], RIGHT),
                (pl.ds(3 * b, b), got.at[p, 1], LEFT),
                (pl.ds(2 * b, b), more.at[p, 0], ACROSS),
            )[kind]
        else:
            src, dst, step = (
                (pl.ds(b + h, b), got.at[p, 0], RIGHT),
                (pl.ds(2 * b + h, b), got.at[p, 1], LEFT),
                (pl.ds(b, h), more.at[p, 0], RIGHT),
                (pl.ds(3 * b + h, h), more.at[p, 1], LEFT),
            )[kind]
        return pltpu.make_async_remote_copy(
            src_ref=buf.at[src], dst_ref=dst, send_sem=self.sends[phase].at[kind, p], recv_sem=self.recvs[phase].at[kind, p],
            device_id=peer(self.me, self.core, self.axes[phase], step), device_id_type=MESH)

    def begin(self, phase, slot):
        if self.slots > self.depth(phase):
            pl.when(slot >= self.depth(phase))(lambda: spend(self.credit, phase, self.direct[phase]))
        for kind in range(3 if self.direct[phase] else 2):
            self.copy(phase, slot, kind).start()

    def middle(self, phase, slot):
        p = lax.rem(slot, self.depth(phase))
        buf, got = self.ins[phase], self.gots[phase]
        b = buf.shape[1] // 4
        h = b // 2
        for kind, base, skip in ((0, b, h), (1, 3 * b + h, 0)):
            self.copy(phase, slot, kind).wait_recv()

            def add(i, n):
                at = pl.ds(base + i, n)
                buf[p, at, :] = (buf[p, at, :].astype(f32) + got[p, kind, pl.ds(skip + i, n), :].astype(f32)).astype(bf16)
            tiles(h, add)
            self.copy(phase, slot, kind + 2).start()

    def finish(self, phase, slot, put):
        p = lax.rem(slot, self.depth(phase))
        buf, got, more = self.ins[phase], self.gots[phase], self.mores[phase]
        b = buf.shape[1] // 4
        h = b // 2
        if self.direct[phase]:
            for kind in range(3):
                self.copy(phase, slot, kind).wait_recv()

            def add_all(at, n):
                value = ((buf[p, pl.ds(at, n), :].astype(f32) + got[p, 0, pl.ds(at, n), :].astype(f32))
                         + (got[p, 1, pl.ds(at, n), :].astype(f32) + more[p, 0, pl.ds(at, n), :].astype(f32)))
                put(at, n, value)
            tiles(b, add_all)
            return
        for kind, base, skip in ((0, 0, h), (1, h, 0)):
            self.copy(phase, slot, kind + 2).wait_recv()

            def add(i, n):
                at = base + i
                value = (buf[p, pl.ds(at, n), :].astype(f32) + got[p, 1 - kind, pl.ds(skip + i, n), :].astype(f32)
                         + more[p, kind, pl.ds(i, n), :].astype(f32))
                put(at, n, value.astype(bf16))
            tiles(h, add)

    def close(self, phase, slot):
        for kind in range(3 if self.direct[phase] else 4):
            self.copy(phase, slot, kind).wait_send()
        if self.slots > self.depth(phase):
            pl.when(slot + self.depth(phase) < self.slots)(
                lambda: grant(self.me, self.core, self.credit, phase, self.axes[phase], self.direct[phase]))


def combine_kernel(own_ref, other_ref, down_hbm, pick_ref, out_ref, down_ref, load_sem, credit, *rest):
    rest = list(rest)

    def take(n):
        taken = rest[:n]
        del rest[:n]
        return taken

    me, core = place()
    partner = {"aa": me["z"] * 2 + (1 - core)}
    quarter = out_ref.shape[1]
    order = (0, 1, 2, 3)

    def load(s, slot, part):
        q = lax.rem(me["y"] + part, 4) if s < PACKED else part
        at = slot + STREAMS[s][1]
        return pltpu.make_async_copy(
            down_hbm.at[:, pl.ds(pl.multiple_of(q * quarter + at * TILE, TILE), TILE)],
            down_ref.at[at, :, pl.ds(part * TILE, TILE)], load_sem.at[at, part])

    greet(me, core)
    for slot in range(max(slots for _, _, slots in STREAMS)):
        for s in order:
            if slot < STREAMS[s][2]:
                for part in range(4):
                    load(s, slot, part).start()
    meet()
    rings, wares = [], []
    for s, (axes, _, slots) in enumerate(STREAMS):
        rings.append(Reduce(me, core, axes[::-1], (False, False, True), take(3), take(3), take(3), take(3), take(3), credit.at[s], slots))
        wares.append(take(6 if s < PACKED else 4))

    def pair(s, slot):
        p = lax.rem(slot, 2)
        if s < PACKED:
            _, src, got, _, send, recv = wares[s]
            dst = got.at[p]
        else:
            src, got, send, recv = wares[s]
            dst = got.at[p, :, pl.ds(80, 80)]
        return pltpu.make_async_remote_copy(
            src_ref=src, dst_ref=dst, send_sem=send.at[0], recv_sem=recv.at[p], device_id=partner, device_id_type=MESH)

    def tile_of(s, slot):
        return pl.multiple_of((slot + STREAMS[s][1]) * TILE, TILE)

    def project(s, slot):
        for part in range(4):
            load(s, slot, part).wait()
        w = down_ref[slot + STREAMS[s][1]]
        mine = jnp.dot(own_ref[...], w, preferred_element_type=f32).astype(bf16)
        if s < PACKED:
            for part in range(4):
                wares[s][0][part] = mine[:, part * TILE:(part + 1) * TILE]
        else:
            wares[s][1][lax.rem(slot, 2), :, 0:80, :] = mine.reshape(8, 80, 4 * TILE)
        pl.when(slot >= 1)(lambda: pair(s, slot - 1).wait_send())
        theirs = jnp.dot(other_ref[...], w, preferred_element_type=f32).astype(bf16)
        if s < PACKED:
            for part in range(4):
                wares[s][1][part] = theirs[:, part * TILE:(part + 1) * TILE]
        else:
            wares[s][0][...] = theirs.reshape(8, 80, 4 * TILE)
        pair(s, slot).start()
        pl.when(slot == rings[s].slots - 1)(lambda: pair(s, slot).wait_send())

    def spread(n, rows):
        return lax.dot_general(pick_ref[n], rows, (((0,), (0,)), ((), ())), preferred_element_type=f32).astype(bf16)

    def launch(s, slot):
        ring = rings[s]
        p, d = lax.rem(slot, ring.depth(0)), lax.rem(slot, 2)
        first_in = ring.ins[0]
        pair(s, slot).wait_recv()
        if s < PACKED:
            own, _, got = wares[s][:3]

            @pl.loop(0, 4)
            def _(part):
                at = pl.multiple_of(part * 1280, 1280)
                first_in[p, pl.ds(at, 640), :] = own[part]
                first_in[p, pl.ds(at + 640, 640), :] = got[d, part]
        else:
            weights = {axis: 4 ** (2 - i) for i, axis in enumerate(ring.axes)}

            @pl.loop(0, 8)
            def _(n):
                rows = spread(n, wares[s][1][d, n])
                for half in range(2):
                    for q in range(4):
                        at = block_at(me, weights, {"z": n // 2, "x": lax.rem(n, 2) * 2 + half, "y": q})
                        first_in[p, pl.ds(at, 128), :] = rows[half * 128:half * 128 + 128, q * TILE:(q + 1) * TILE]
        ring.begin(0, slot)

    def pass_on(s, phase, slot):
        ring = rings[s]
        dst, p = ring.ins[phase + 1], lax.rem(slot, 2)
        if phase == 0 and s < PACKED:
            summed = wares[s][3]

            def hold(at, n, value):
                summed[pl.ds(at, n), :] = value
            ring.finish(0, slot, hold)
            weights = {ring.axes[1]: 4, ring.axes[2]: 1}

            @pl.loop(0, 8)
            def _(n):
                at = pl.multiple_of(n * 80, 16)
                rows = spread(n, jnp.concatenate([summed[pl.ds(at, 80), :], summed[pl.ds(at + 640, 80), :]], axis=0))
                for half in range(2):
                    at = block_at(me, weights, {"z": n // 2, "x": lax.rem(n, 2) * 2 + half})
                    dst[p, pl.ds(at, 128), :] = rows[half * 128:half * 128 + 128]
        else:
            def put(at, n, value):
                dst[p, pl.ds(at, n), :] = value
            ring.finish(phase, slot, put)
        ring.begin(phase + 1, slot)
        ring.close(phase, slot)

    def deliver(s, slot):
        def put(at, n, value):
            out_ref[pl.ds(at, n), pl.ds(tile_of(s, slot), TILE)] = value
        rings[s].finish(2, slot, put)
        rings[s].close(2, slot)

    def stage(step, delay, body, lowest=0, streams=range(len(STREAMS))):
        for s in streams:
            slot = step - delay
            pl.when((slot >= lowest) & (slot < STREAMS[s][2]))(functools.partial(body, s, slot))

    start = jnp.int32(0)
    project(order[0], start)
    for before, s in zip(order, order[1:]):
        project(s, start)
        launch(before, start)
    launch(order[-1], start)
    packed, plain = range(PACKED), range(PACKED, len(STREAMS))

    @pl.loop(0, max(slots for _, _, slots in STREAMS) + 5)
    def _(step):
        stage(step, 1, lambda s, slot: rings[s].middle(0, slot))
        stage(step, 0, launch, 1, packed)
        stage(step, 3, lambda s, slot: rings[s].middle(1, slot))
        stage(step, 5, deliver)
        stage(step, 4, lambda s, slot: pass_on(s, 1, slot))
        for s in plain:
            stage(step, 2, lambda s, slot: pass_on(s, 0, slot), 0, (s,))
            stage(step, 0, launch, 1, (s,))
        stage(step, 2, lambda s, slot: pass_on(s, 0, slot), 0, packed)
        stage(step, -1, project, 1)


def combine(own, other, down, pick):
    quarter = down.shape[1] // 4
    vmem = pl.BlockSpec(memory_space=pltpu.VMEM)
    dma = pltpu.SemaphoreType.DMA
    count = quarter // TILE
    scratch = [pltpu.VMEM((count, down.shape[0], 4 * TILE), bf16), dma((count, 4)), pltpu.SemaphoreType.REGULAR((len(STREAMS), 3, 3))]
    for s in range(len(STREAMS)):
        sizes = (5120 if s < PACKED else 8192, 2048, 512)
        depths = (3 if s < PACKED else 2, 2, 2)
        scratch += [rows_buffer(d, n) for d, n in zip(depths, sizes)]
        scratch += [rows_buffer(d, 2, n // 4) for d, n in zip(depths, sizes)]
        scratch += [rows_buffer(depths[0], 2, sizes[0] // 8), rows_buffer(2, 2, sizes[1] // 8), rows_buffer(2, 1, sizes[2] // 4)]
        scratch += [dma((4, d)) for d in depths] * 2
        if s < PACKED:
            scratch += [rows_buffer(4, 640), rows_buffer(4, 640), rows_buffer(2, 4, 640), rows_buffer(1280), dma((1,)), dma((2,))]
        else:
            scratch += [pltpu.VMEM((8, 80, 512), bf16), pltpu.VMEM((2, 8, 160, 512), bf16), dma((1,)), dma((2,))]
    return pl.pallas_call(
        combine_kernel,
        out_shape=jax.ShapeDtypeStruct((128, quarter), f32),
        in_specs=[vmem, vmem, pl.BlockSpec(memory_space=pl.ANY), vmem],
        out_specs=vmem,
        scratch_shapes=scratch,
        compiler_params=pltpu.CompilerParams(collective_id=1, has_side_effects=True, vmem_limit_bytes=66900000),
        name="combine",
    )(own, other, down, pick)


def on_device(tokens, routing, gate_codes, w_gate, w_up, w_down):
    own, other, pick = dispatch(tokens, routing.T, gate_codes.T, w_gate[0], w_up[0])
    return combine(own, other, w_down[0], pick).astype(bf16)


def solution(mesh):
    return jax.shard_map(
        on_device,
        mesh=mesh,
        in_specs=(
            P(("aa", "col"), "ba"),
            P(("aa", "col"), None),
            P(("aa", "col"), None),
            P(("aa", "col"), None, "ba"),
            P(("aa", "col"), None, "ba"),
            P(("aa", "col"), "ba", None),
        ),
        out_specs=P(("aa", "col"), "ba"),
        check_vma=False,
    )
```
